32 devices in a mesh: dp: 1 (over z), sp: 32 (over y, x, core).
Axes of the slice: x: 4, y: 4, z: 1, core: 2. Of those that a mesh axis runs over, the one named last changes fastest.
The devices are a block of a 4x4x8 slice.
Arguments:
- x: bfloat16 [16, 2048], P('dp')
- lens: int32 [16], P('dp')
- wq: bfloat16 [2, 2048, 2048], replicated
- wk: bfloat16 [2, 2048, 256], replicated
- wv: bfloat16 [2, 2048, 256], replicated
- wo: bfloat16 [2, 2048, 2048], P(None, 'sp')
- w1: bfloat16 [2, 2048, 8192], P(None, None, 'sp')
- w2: bfloat16 [2, 8192, 2048], P(None, 'sp')
- g1: bfloat16 [2, 2048], replicated
- g2: bfloat16 [2, 2048], replicated
- kc: bfloat16 [2, 16, 16384, 4, 64], P(None, 'dp', 'sp')
- vc: bfloat16 [2, 16, 16384, 4, 64], P(None, 'dp', 'sp')
Outputs:
- output 1: bfloat16 [16, 2048], P('dp')
- output 2: bfloat16 [2, 16, 16384, 4, 64], P(None, 'dp', 'sp')
- output 3: bfloat16 [2, 16, 16384, 4, 64], P(None, 'dp', 'sp')
All inputs are finite; a program needn't handle non-finite values.
Results may differ from the reference program's by a relative error of at most 0.00880827.
Values are sent between devices in bfloat16 or wider.
A program may use at most 768 MiB of HBM per device.

```python
import math
import jax
import jax.numpy as jnp
from jax import lax

B = 16
S_DEV = 512
SEQ = 32
D = 2048
HEADS = 32
KV_HEADS = 4
HEAD = 64
LAYERS = 2
S = S_DEV * SEQ
G = HEADS // KV_HEADS
FF = 4 * D
BLOCK = min(S_DEV, 1024)
EPS = 1e-6


def _rms(h, g):
    r = lax.rsqrt(jnp.mean(h * h, axis=-1, keepdims=True) + EPS)
    return (h * r * g.astype(jnp.float32)).astype(jnp.bfloat16)


def _mm(a, w):
    return jnp.dot(a, w, preferred_element_type=jnp.float32)


def _cache(key, t):
    k = jax.random.split(key, 7)
    ph = jax.random.uniform(k[0], (B, 3), jnp.float32)
    fr = jax.random.uniform(k[1], (B, 3), jnp.float32, 1.0, 3.0)
    wave = jnp.sin(2.0 * math.pi * (fr[:, None, :] * t[None, :, None] + ph[:, None, :]))
    kdir = jax.random.normal(k[2], (B, 1, KV_HEADS, HEAD), jnp.float32)
    u1 = jax.random.normal(k[3], (B, 1, KV_HEADS, HEAD), jnp.float32)
    u2 = jax.random.normal(k[4], (B, 1, KV_HEADS, HEAD), jnp.float32)
    kc = jax.random.normal(k[5], (B, S, KV_HEADS, HEAD), jnp.float32) + wave[:, :, 0, None, None] * kdir
    vc = (0.5 * jax.random.normal(k[6], (B, S, KV_HEADS, HEAD), jnp.float32)
          + wave[:, :, 1, None, None] * u1 + wave[:, :, 2, None, None] * u2)
    return kc.astype(jnp.bfloat16), vc.astype(jnp.bfloat16)


def _lengths(key):
    draws = jax.random.randint(key, (B,), 0, 256, dtype=jnp.int32)
    scaled = draws * (S - 1) // 255
    lens = scaled * draws // 255 + 1
    return lens.at[0].set(S).astype(jnp.int32)


def setup_inputs(seed: int = 0, part: int = 0) -> dict:
    key = jax.random.key(seed)
    ks = jax.random.split(key, 8)
    kp = jax.random.split(jax.random.fold_in(key, part), 3)
    gamma = (math.log(S) - 1.0) / math.sqrt(HEAD)
    wk = jax.random.normal(ks[0], (LAYERS, D, KV_HEADS, 1, HEAD), jnp.float32) * D ** -0.5
    wq = gamma * wk + jax.random.normal(ks[1], (LAYERS, D, KV_HEADS, G, HEAD), jnp.float32) * D ** -0.5
    wv = jax.random.normal(ks[2], (LAYERS, D, KV_HEADS * HEAD), jnp.float32) * D ** -0.5
    wo = jax.random.normal(ks[3], (LAYERS, HEADS * HEAD, D), jnp.float32) * (HEADS * HEAD) ** -0.5
    w1 = jax.random.normal(ks[4], (LAYERS, D, FF), jnp.float32) * D ** -0.5
    w2 = jax.random.normal(ks[5], (LAYERS, FF, D), jnp.float32) * FF ** -0.5
    g1 = 1.0 + 0.1 * jax.random.normal(ks[6], (LAYERS, D), jnp.float32)
    g2 = 1.0 + 0.1 * jax.random.normal(ks[7], (LAYERS, D), jnp.float32)
    t = jnp.arange(S, dtype=jnp.float32) / S
    ck = jax.random.split(kp[2], LAYERS)
    caches = [_cache(ck[i], t) for i in range(LAYERS)]
    bf = jnp.bfloat16
    return {
        'x': jax.random.normal(kp[0], (B, D), jnp.float32).astype(bf),
        'lens': _lengths(kp[1]),
        'wq': wq.reshape(LAYERS, D, HEADS * HEAD).astype(bf),
        'wk': wk.reshape(LAYERS, D, KV_HEADS * HEAD).astype(bf),
        'wv': wv.astype(bf),
        'wo': wo.astype(bf),
        'w1': w1.astype(bf),
        'w2': w2.astype(bf),
        'g1': g1.astype(bf),
        'g2': g2.astype(bf),
        'kc': jnp.stack([c[0] for c in caches]),
        'vc': jnp.stack([c[1] for c in caches]),
    }


def _attend(q, kc, vc, lens):
    qf = q.astype(jnp.float32)

    def body(carry, i):
        m, l, o = carry
        k = lax.dynamic_slice_in_dim(kc, i * BLOCK, BLOCK, axis=1).astype(jnp.float32)
        v = lax.dynamic_slice_in_dim(vc, i * BLOCK, BLOCK, axis=1).astype(jnp.float32)
        s = jnp.einsum('bkgd,bskd->bkgs', qf, k) * HEAD ** -0.5
        posn = i * BLOCK + jnp.arange(BLOCK)
        s = jnp.where((posn[None, :] < lens[:, None])[:, None, None, :], s, -jnp.inf)
        mn = jnp.maximum(m, jnp.max(s, axis=-1))
        c = jnp.exp(m - mn)
        p = jnp.exp(s - mn[..., None])
        o = o * c[..., None] + jnp.einsum('bkgs,bskd->bkgd', p, v)
        return (mn, l * c + jnp.sum(p, axis=-1), o), None

    init = (jnp.full((B, KV_HEADS, G), -jnp.inf, jnp.float32),
            jnp.zeros((B, KV_HEADS, G), jnp.float32),
            jnp.zeros((B, KV_HEADS, G, HEAD), jnp.float32))
    (m, l, o), _ = lax.scan(body, init, jnp.arange(S // BLOCK))
    return o / l[..., None]


def reference(x, lens, wq, wk, wv, wo, w1, w2, g1, g2, kc, vc):
    posn = jnp.arange(S)
    write = (posn[None, :] == (lens - 1)[:, None])[:, :, None, None]

    def layer(h, w):
        wq_, wk_, wv_, wo_, w1_, w2_, g1_, g2_, kc_, vc_ = w
        xn = _rms(h, g1_)
        q = _mm(xn, wq_).astype(jnp.bfloat16).reshape(B, KV_HEADS, G, HEAD)
        k = _mm(xn, wk_).astype(jnp.bfloat16).reshape(B, 1, KV_HEADS, HEAD)
        v = _mm(xn, wv_).astype(jnp.bfloat16).reshape(B, 1, KV_HEADS, HEAD)
        kn = jnp.where(write, k, kc_)
        vn = jnp.where(write, v, vc_)
        o = _attend(q, kn, vn, lens).astype(jnp.bfloat16).reshape(B, HEADS * HEAD)
        h = h + _mm(o, wo_)
        u = jax.nn.gelu(_mm(_rms(h, g2_), w1_)).astype(jnp.bfloat16)
        h = h + _mm(u, w2_)
        return h, (kn, vn)

    h, (kn, vn) = lax.scan(layer, x.astype(jnp.float32), (wq, wk, wv, wo, w1, w2, g1, g2, kc, vc))
    return h.astype(jnp.bfloat16), kn, vn
```

```python
import functools

import jax
import jax.numpy as jnp
from jax import lax
from jax.experimental import pallas as pl
from jax.experimental.pallas import tpu as pltpu
from jax.sharding import PartitionSpec as P

EPS = 1e-6
LANES = 128
SUB = 8
NEG = float(jnp.finfo(jnp.float32).min)
F32 = jnp.float32
BF16 = jnp.bfloat16
MESH = pl.DeviceIdType.MESH
QCH = 4


def _dot(a, w):
    return jnp.dot(a, w, preferred_element_type=F32)


def _step_kernel(n, dims, lens_ref, x_ref, g1_ref, g2_ref, wq, wk, wv, wo, w1, w2, kc, vc,
                 y_ref, kn_out, vn_out,
                 wq_v, wk_v, wv_v, wo_v, w1_v, w2_v, k_v, v_v, qs, kn, vn, xn, hb, hown,
                 asend, arecv, s1, r1, s2, r2, lsem, ssem, rsem):
    nl, nb, s_dev, kvd, dh = dims
    D = x_ref.shape[1]
    nc = n // 2
    me = lax.axis_index('sp')
    par = lax.rem(me, 2)
    half = nb // 2

    cw = D // QCH

    def loads(l):
        out = {}
        i = 0

        def add(name, src, dst):
            nonlocal i
            out[name] = pltpu.make_async_copy(src, dst, lsem.at[l, i])
            i += 1
        add('wk', wk.at[l], wk_v.at[l])
        add('wv', wv.at[l], wv_v.at[l])
        for j in range(QCH):
            add(f'wq{j}', wq.at[l, :, pl.ds(j * cw, cw)], wq_v.at[l, :, pl.ds(j * cw, cw)])
        for j in range(2):
            add(f'k{j}', kc.at[l, pl.ds(j * half, half)], k_v.at[l, pl.ds(j * half, half)])
            add(f'v{j}', vc.at[l, pl.ds(j * half, half)], v_v.at[l, pl.ds(j * half, half)])
        add('wo', wo.at[l], wo_v.at[l, pl.ds(pl.multiple_of(par * dh, dh), dh)])
        add('w1', w1.at[l], w1_v.at[l])
        add('w2', w2.at[l], w2_v.at[l])
        return out

    ld = [loads(l) for l in range(nl)]
    for c in ld[0].values():
        c.start()

    bar = pltpu.get_barrier_semaphore()

    def sig(k, carry):
        pl.semaphore_signal(bar, 1, device_id={'sp': lax.rem(me + k, n)}, device_id_type=MESH)
        return carry
    lax.fori_loop(1, n, sig, 0)

    def send_all(src_of, dst, phase, step=1):
        def body(k, carry):
            d = lax.rem(me + k * step, n)
            pltpu.make_async_remote_copy(src_of(d), dst, ssem.at[phase], rsem.at[phase],
                                         device_id={'sp': d}, device_id_type=MESH).start()
            return carry
        lax.fori_loop(1, n // step, body, 0)

    def wait_recv(buf, count, phase):
        r = buf.at[pl.ds(0, count)]
        pltpu.make_async_copy(r, r, rsem.at[phase]).wait()

    def wait_send(buf, count, phase):
        r = buf.at[pl.ds(0, count)]
        pltpu.make_async_copy(r, r, ssem.at[phase]).wait()

    lane = lax.broadcasted_iota(jnp.int32, (SUB, LANES), 1)
    row = lax.broadcasted_iota(jnp.int32, (SUB, LANES), 0)
    lo = lane < dh
    quart = lax.rem(lane, dh) < dh // 2
    ma = (row < SUB // 2) & lo
    mb = (row >= SUB // 2) & (~lo)
    col = lax.broadcasted_iota(jnp.int32, (2 * nc, s_dev), 1)
    off = me * s_dev

    def rms_to_xn(st, g_ref, l):
        for r in range(2):
            ss = None
            for c in range(nc):
                t = hb[st, 2 * c + r]
                ss = t * t if ss is None else ss + t * t
            rr = lax.rsqrt(jnp.sum(ss, axis=1, keepdims=True) / D + EPS)
            for c in range(nc):
                g = g_ref[l:l + 1, c * LANES:(c + 1) * LANES].astype(F32)
                xn[r * SUB:(r + 1) * SUB, c * LANES:(c + 1) * LANES] = (hb[st, 2 * c + r] * rr * g).astype(BF16)

    for c in range(nc):
        for r in range(2):
            hb[0, 2 * c + r] = x_ref[r * SUB:(r + 1) * SUB, c * LANES:(c + 1) * LANES].astype(F32)
    h = hb[0, me]

    ph = 0
    st = 0
    for l in range(nl):
        rms_to_xn(st, g1_ref, l)
        ld[l]['wk'].wait()
        ld[l]['wv'].wait()
        kn[...] = _dot(xn[...], wk_v[l]).astype(BF16).astype(F32)
        vn[...] = _dot(xn[...], wv_v[l]).astype(BF16).astype(F32)
        for j in range(QCH):
            ld[l][f'wq{j}'].wait()
            q = _dot(xn[...], wq_v[l, :, j * cw:(j + 1) * cw]).astype(BF16).astype(F32)
            for t in range(cw // LANES):
                c = j * (cw // LANES) + t
                for r in range(2):
                    qs[pl.ds(r * SUB * nc + c, SUB, stride=nc), :] = q[r * SUB:(r + 1) * SUB, t * LANES:(t + 1) * LANES]

        for r in range(2):
            ld[l][f'k{r}'].wait()
            ld[l][f'v{r}'].wait()
            for bb in range(half):
                b = r * half + bb
                xq = qs[b * nc:(b + 1) * nc, :]
                xr = pltpu.roll(xq, dh, 1)
                z = jnp.zeros((SUB, LANES), F32)
                parts = []
                for a, o in ((xq, xr), (xr, xq)):
                    e0 = jnp.where(ma, a[0:SUB], jnp.where(mb, o[0:SUB], 0.0))
                    e1 = jnp.where(ma, a[SUB:], jnp.where(mb, o[SUB:], 0.0))
                    parts.append(jnp.concatenate([e0, z], axis=1))
                    parts.append(jnp.concatenate([z, e1], axis=1))
                qf = jnp.concatenate(parts, axis=0)
                pb = lens_ref[b] - 1 - off
                s = _dot(qf.astype(BF16), k_v[l, b]) * dh ** -0.5
                sn = jnp.sum(qf * kn[b:b + 1, :], axis=1, keepdims=True) * dh ** -0.5
                s = jnp.where(col < pb, s, jnp.where(col == pb, sn, -jnp.inf))
                m = jnp.maximum(jnp.max(s, axis=1, keepdims=True), NEG)
                p = jnp.exp(s - m)
                den = jnp.sum(p, axis=1, keepdims=True)
                inside = jnp.logical_and(pb >= 0, pb < s_dev)
                pn = jnp.where(inside, jnp.exp(sn - m), 0.0)
                pz = jnp.where(col == pb, 0.0, p).astype(BF16)
                o = lax.dot_general(pz, v_v[l, b], (((1,), (1,)), ((), ())), preferred_element_type=F32)
                o = o + pn * vn[b:b + 1, :]
                for t in range(2):
                    ev = o[t * SUB:(t + 1) * SUB, t * LANES:(t + 1) * LANES]
                    od = o[nc + t * SUB:nc + (t + 1) * SUB, t * LANES:(t + 1) * LANES]
                    evr = pltpu.roll(ev, dh, 1)
                    odr = pltpu.roll(od, dh, 1)
                    tile = jnp.where(row < SUB // 2, jnp.where(lo, ev, odr), jnp.where(lo, evr, od))
                    me_, le_ = m[t * SUB:(t + 1) * SUB], den[t * SUB:(t + 1) * SUB]
                    mo_, lo_ = m[nc + t * SUB:nc + (t + 1) * SUB], den[nc + t * SUB:nc + (t + 1) * SUB]
                    stat = jnp.where(lo, jnp.where(quart, me_, le_), jnp.where(quart, mo_, lo_))
                    base = (2 * SUB * t + r) * 2 * SUB + bb
                    asend[l, pl.ds(base, SUB, stride=4 * SUB), :] = tile
                    asend[l, pl.ds(base + SUB, SUB, stride=4 * SUB), :] = stat
        if l == 0:
            pl.semaphore_wait(bar, n - 1)
        send_all(lambda d: asend.at[l, pl.ds(pl.multiple_of(d * 2 * SUB, 2 * SUB), 2 * SUB)], arecv.at[l, me], ph)
        if l == 0:
            other = me + 1 - 2 * par
            wo_x = []
            for ll in range(nl):
                cp = pltpu.make_async_remote_copy(
                    wo.at[ll], wo_v.at[ll, pl.ds(pl.multiple_of(par * dh, dh), dh)],
                    ssem.at[5 * nl + ll], rsem.at[5 * nl + ll], device_id={'sp': other}, device_id_type=MESH)
                cp.start()
                wo_x.append(cp)
            for cp in ld[1].values():
                cp.start()
        arecv[l, me] = asend[l, pl.ds(pl.multiple_of(me * 2 * SUB, 2 * SUB), 2 * SUB), :]
        pad = jnp.zeros((LANES - nb, kvd), F32)
        kn_out[l] = jnp.concatenate([kn[...], pad], axis=0).T
        vn_out[l] = jnp.concatenate([vn[...], pad], axis=0).T
        wait_recv(arecv.at[l], n - 1, ph)
        ph += 1

        mx = None
        for i in range(n):
            sa = arecv[l, i, SUB:]
            mt = jnp.where(quart, sa, pltpu.roll(sa, dh // 2, 1))
            mx = mt if mx is None else jnp.maximum(mx, mt)
        num = jnp.zeros((SUB, LANES), F32)
        den = jnp.zeros((SUB, LANES), F32)
        for i in range(n):
            sa = arecv[l, i, SUB:]
            mt = jnp.where(quart, sa, pltpu.roll(sa, dh // 2, 1))
            dt = jnp.where(quart, pltpu.roll(sa, LANES - dh // 2, 1), sa)
            w = jnp.exp(mt - mx)
            den = den + w * dt
            num = num + w * arecv[l, i, 0:SUB]
        att = (num / den).astype(BF16)

        ld[l]['wo'].wait()
        wo_x[l].wait()
        part = _dot(att, wo_v[l])
        for c in range(nc):
            s1[l, c] = part[:, c * LANES:(c + 1) * LANES]
        mc = lax.div(me, 2)
        send_all(lambda d: s1.at[l, lax.div(d, 2)], r1.at[l, mc], ph, 2)
        r1[l, mc] = s1[l, mc]
        wait_recv(r1.at[l], nc - 1, ph)
        ph += 1
        tot = r1[l, 0]
        for c in range(1, nc):
            tot = tot + r1[l, c]
        h = h + tot

        def gather(h):
            hown[st] = h
            send_all(lambda d: hown.at[st], hb.at[st + 1, me], ph)
            hb[st + 1, me] = h
            wait_recv(hb.at[st + 1], n - 1, ph)
        gather(h)
        ph += 1
        st += 1

        rms_to_xn(st, g2_ref, l)
        ld[l]['w1'].wait()
        u = jax.nn.gelu(_dot(xn[...], w1_v[l]), approximate=True).astype(BF16)
        ld[l]['w2'].wait()
        part = _dot(u, w2_v[l])
        for c in range(nc):
            for r in range(2):
                s2[l, 2 * c + r] = part[r * SUB:(r + 1) * SUB, c * LANES:(c + 1) * LANES]
        send_all(lambda d: s2.at[l, d], r2.at[l, me], ph)
        r2[l, me] = s2[l, me]
        wait_recv(r2.at[l], n - 1, ph)
        ph += 1
        tot = r2[l, 0]
        for d in range(1, n):
            tot = tot + r2[l, d]
        h = h + tot
        gather(h)
        ph += 1
        st += 1

    for c in range(nc):
        for r in range(2):
            y_ref[r * SUB:(r + 1) * SUB, c * LANES:(c + 1) * LANES] = hb[st, 2 * c + r].astype(BF16)

    for l in range(nl):
        wait_send(arecv.at[l], n - 1, 5 * l)
        wait_send(r1.at[l], nc - 1, 5 * l + 1)
        wait_send(hb.at[0], n - 1, 5 * l + 2)
        wait_send(r2.at[l], n - 1, 5 * l + 3)
        wait_send(hb.at[0], n - 1, 5 * l + 4)


def _cache_kernel(s_dev, per, lens_ref, y_ref, kn_ref, vn_ref, k_ref, v_ref, y_out, k_out, v_out):
    off = lax.axis_index('sp') * s_dev
    g = pl.program_id(1)
    y_out[...] = y_ref[...]
    lane = lax.broadcasted_iota(jnp.int32, kn_ref.shape[1:], 1)
    col = lax.broadcasted_iota(jnp.int32, k_ref.shape[2:], 1)
    for i in range(per):
        b = g * per + i
        pb = lens_ref[b] - 1 - off
        for new, src, dst in ((kn_ref, k_ref, k_out), (vn_ref, v_ref, v_out)):
            c = jnp.sum(jnp.where(lane == b, new[0], 0.0), axis=1, keepdims=True)
            dst[0, i] = jnp.where(col == pb, c, src[0, i].astype(F32)).astype(BF16)


def solution(mesh):
    n = mesh.shape['sp']
    kspec = P(None, 'dp', 'sp', None, None)

    def local(x, lens, wq, wk, wv, wo, w1, w2, g1, g2, kc, vc):
        nl, nb, s_dev, kvh, dh = kc.shape
        D = x.shape[1]
        kvd = kvh * dh
        ff = w1.shape[2]
        nc = n // 2
        kt = jnp.transpose(kc, (0, 1, 3, 4, 2)).reshape(nl, nb, kvd, s_dev)
        vt = jnp.transpose(vc, (0, 1, 3, 4, 2)).reshape(nl, nb, kvd, s_dev)
        vm = pl.BlockSpec(memory_space=pltpu.VMEM)
        anys = pl.BlockSpec(memory_space=pl.ANY)
        y, kn, vn = pl.pallas_call(
            functools.partial(_step_kernel, n, (nl, nb, s_dev, kvd, dh)),
            out_shape=(jax.ShapeDtypeStruct((nb, D), BF16),
                       jax.ShapeDtypeStruct((nl, kvd, LANES), F32),
                       jax.ShapeDtypeStruct((nl, kvd, LANES), F32)),
            in_specs=[pl.BlockSpec(memory_space=pltpu.SMEM), vm, vm, vm] + [anys] * 8,
            out_specs=(vm, vm, vm),
            scratch_shapes=[
                pltpu.VMEM((nl, D, D), BF16),
                pltpu.VMEM((nl, D, kvd), BF16),
                pltpu.VMEM((nl, D, kvd), BF16),
                pltpu.VMEM((nl, 2 * dh, D), BF16),
                pltpu.VMEM((nl, D, ff), BF16),
                pltpu.VMEM((nl, ff, D), BF16),
                pltpu.VMEM((nl, nb, kvd, s_dev), BF16),
                pltpu.VMEM((nl, nb, kvd, s_dev), BF16),
                pltpu.VMEM((nb * nc, LANES), F32),
                pltpu.VMEM((nb, kvd), F32),
                pltpu.VMEM((nb, kvd), F32),
                pltpu.VMEM((nb, D), BF16),
                pltpu.VMEM((2 * nl + 1, n, SUB, LANES), F32),
                pltpu.VMEM((2 * nl, SUB, LANES), F32),
                pltpu.VMEM((nl, n * 2 * SUB, LANES), F32),
                pltpu.VMEM((nl, n, 2 * SUB, LANES), F32),
                pltpu.VMEM((nl, nc, SUB, LANES), F32),
                pltpu.VMEM((nl, nc, SUB, LANES), F32),
                pltpu.VMEM((nl, n, SUB, LANES), F32),
                pltpu.VMEM((nl, n, SUB, LANES), F32),
                pltpu.SemaphoreType.DMA((nl, QCH + 9)),
                pltpu.SemaphoreType.DMA((6 * nl,)),
                pltpu.SemaphoreType.DMA((6 * nl,)),
            ],
            compiler_params=pltpu.CompilerParams(
                collective_id=0, has_side_effects=True, vmem_limit_bytes=60 * 1024 * 1024),
        )(lens, x, g1, g2, wq, wk, wv, wo, w1, w2, kt, vt)

        per = 2
        cspec = pl.BlockSpec((1, per, kvd, s_dev), lambda l, g: (l, g, 0, 0))
        nspec = pl.BlockSpec((1, kvd, LANES), lambda l, g: (l, 0, 0))
        yspec = pl.BlockSpec((nb, D), lambda l, g: (0, 0))
        y, k2, v2 = pl.pallas_call(
            functools.partial(_cache_kernel, s_dev, per),
            out_shape=(jax.ShapeDtypeStruct((nb, D), BF16), jax.ShapeDtypeStruct(kt.shape, BF16),
                       jax.ShapeDtypeStruct(vt.shape, BF16)),
            grid=(nl, nb // per),
            in_specs=[pl.BlockSpec(memory_space=pltpu.SMEM), yspec, nspec, nspec, cspec, cspec],
            out_specs=(yspec, cspec, cspec),
        )(lens, y, kn, vn, kt, vt)

        def back(a):
            return jnp.transpose(a.reshape(nl, nb, kvh, dh, s_dev), (0, 1, 4, 2, 3))
        return y, back(k2), back(v2)

    return jax.shard_map(
        local, mesh=mesh,
        in_specs=(P('dp', None), P('dp'), P(), P(), P(), P(None, 'sp', None), P(None, None, 'sp'),
                  P(None, 'sp', None), P(), P(), kspec, kspec),
        out_specs=(P('dp', None), kspec, kspec), check_vma=False)
```

```python
import functools

import jax
import jax.numpy as jnp
from jax import lax
from jax.experimental import pallas as pl
from jax.experimental.pallas import tpu as pltpu
from jax.sharding import PartitionSpec as P

EPS = 1e-6
LANES = 128
SUB = 8
NEG = float(jnp.finfo(jnp.float32).min)
F32 = jnp.float32
BF16 = jnp.bfloat16
MESH = pl.DeviceIdType.MESH
QCH = 4
OWN = 1
STW = 32


def _dot(a, w):
    return jnp.dot(a, w, preferred_element_type=F32)


def _step_kernel(n, dims, lens, x, g1, g2, wq, wk, wv, wo, w1, w2, kc, vc,
                 y_ref, k_v, v_v,
                 wq_v, wk_v, wv_v, wo_v, w1_v, w2_v, x_v, g1_v, g2_v, lens_v, qs, kn, vn, knt, vnt, xn, hb, hs,
                 os, orv, ss, sr, s1, r1, s2, r2, lsem, ssem, rsem):
    nl, nb, s_dev, kvd, dh = dims
    D = x_v.shape[1]
    nc = n // 2
    me = lax.axis_index('sp')
    par = lax.rem(me, 2)
    mc = lax.div(me, 2)
    own = par == OWN
    other = me + 1 - 2 * par

    cw = D // QCH

    def loads(l):
        out = {}
        i = 0

        def add(name, src, dst):
            nonlocal i
            out[name] = pltpu.make_async_copy(src, dst, lsem.at[l, i])
            i += 1
        if l == 0:
            add('x', x, x_v)
            add('g1', g1, g1_v)
            add('lens', lens, lens_v)
        add('wk', wk.at[l], wk_v.at[l])
        add('wv', wv.at[l], wv_v.at[l])
        for j in range(QCH):
            add(f'wq{j}', wq.at[l, :, pl.ds(j * cw, cw)], wq_v.at[l, :, pl.ds(j * cw, cw)])
        for j in range(2):
            add(f'k{j}', kc.at[l, pl.ds(j * SUB, SUB)], k_v.at[l, pl.ds(j * SUB, SUB)])
            add(f'v{j}', vc.at[l, pl.ds(j * SUB, SUB)], v_v.at[l, pl.ds(j * SUB, SUB)])
        if l == 0:
            add('g2', g2, g2_v)
        add('w1', w1.at[l], w1_v.at[l])
        add('w2', w2.at[l], w2_v.at[l])
        return out

    ld = [loads(l) for l in range(nl)]
    for c in ld[0].values():
        c.start()

    bar = pltpu.get_barrier_semaphore()

    def sig(k, carry):
        pl.semaphore_signal(bar, 1, device_id={'sp': lax.rem(me + k, n)}, device_id_type=MESH)
        return carry
    lax.fori_loop(1, n, sig, 0)

    A2A, STAT, RS1, AG1, RS2, AG2, WO = range(7)

    def sem(l, r, kind):
        return (l * 2 + r) * 7 + kind

    def rcopy(src, dst, i, d):
        return pltpu.make_async_remote_copy(src, dst, ssem.at[i], rsem.at[i], device_id={'sp': d}, device_id_type=MESH)

    def to_owners(pairs):
        def body(k, carry):
            c = lax.rem(mc + k, nc)
            for src, dst, i in pairs:
                rcopy(src(c), dst, i, 2 * c + OWN).start()
            return carry
        lax.fori_loop(1, nc, body, 0)

        @pl.when(jnp.logical_not(own))
        def _():
            body(0, 0)

    def wait(ref, count, s):
        r = ref.at[pl.ds(0, count)]
        pltpu.make_async_copy(r, r, s).wait()

    lane = lax.broadcasted_iota(jnp.int32, (SUB, LANES), 1)
    row = lax.broadcasted_iota(jnp.int32, (SUB, LANES), 0)
    lo = lane < dh
    ma = (row < SUB // 2) & lo
    mb = (row >= SUB // 2) & (~lo)
    col = lax.broadcasted_iota(jnp.int32, (2 * nc, s_dev), 1)
    col1 = lax.broadcasted_iota(jnp.int32, (1, s_dev), 1)
    off = me * s_dev

    def normed(st, r, g_v, l):
        ss_ = None
        for c in range(nc):
            t = hb[st, r, c]
            ss_ = t * t if ss_ is None else ss_ + t * t
        rr = lax.rsqrt(jnp.sum(ss_, axis=1, keepdims=True) / D + EPS)
        for c in range(nc):
            g = g_v[l:l + 1, c * LANES:(c + 1) * LANES].astype(F32)
            xn[r, :, c * LANES:(c + 1) * LANES] = (hb[st, r, c] * rr * g).astype(BF16)

    def gather(l, st, r, kind, h):
        hs[st, r] = h

        def body(k, carry):
            rcopy(hs.at[st, r], hb.at[st + 1, r, mc], sem(l, r, kind), lax.rem(me + k, n)).start()
            return carry
        lax.fori_loop(1, n, body, 0)
        hb[st + 1, r, mc] = h

    def gathered(l, st, r, kind):
        @pl.when(own)
        def _():
            wait(hb.at[st + 1, r], nc - 1, rsem.at[sem(l, r, kind)])

        @pl.when(jnp.logical_not(own))
        def _():
            wait(hb.at[st + 1, r], nc, rsem.at[sem(l, r, kind)])

    def put_new(l, new_t, ref):
        for b in range(nb):
            pb = lens_v[b] - 1 - off
            hit = jnp.where(col1 == pb, 1.0, 0.0).astype(BF16)
            c = jnp.broadcast_to(new_t[:, b:b + 1], (kvd, LANES)).astype(BF16)
            for t in range(s_dev // LANES):
                sl = slice(t * LANES, (t + 1) * LANES)
                hm = jnp.broadcast_to(hit[:, sl], (kvd, LANES)) > 0.5
                ref[l, b, :, sl] = jnp.where(hm, c, ref[l, b, :, sl])

    ld[0]['x'].wait()
    for c in range(nc):
        for r in range(2):
            hb[0, r, c] = x_v[r * SUB:(r + 1) * SUB, c * LANES:(c + 1) * LANES].astype(F32)
    ld[0]['g1'].wait()

    wo_in = [rcopy(wo.at[ll], wo_v.at[ll, pl.ds((1 - OWN) * dh, dh)], sem(ll, 0, WO), other) for ll in range(nl)]
    wo_my = [pltpu.make_async_copy(wo.at[ll], wo_v.at[ll, pl.ds(OWN * dh, dh)], lsem.at[ll, QCH + 12])
             for ll in range(nl)]
    st = 0
    for l in range(nl):
        for r in range(2):
            if l > 0:
                gathered(l - 1, st - 1, r, AG2)
            normed(st, r, g1_v, l)
            if r == 0:
                ld[l]['wk'].wait()
                ld[l]['wv'].wait()
            kn[r] = _dot(xn[r], wk_v[l]).astype(BF16).astype(F32)
            vn[r] = _dot(xn[r], wv_v[l]).astype(BF16).astype(F32)
            for j in range(QCH):
                if r == 0:
                    ld[l][f'wq{j}'].wait()
                q = _dot(xn[r], wq_v[l, :, j * cw:(j + 1) * cw]).astype(BF16).astype(F32)
                for t in range(cw // LANES):
                    qs[r, pl.ds(j * (cw // LANES) + t, SUB, stride=nc), :] = q[:, t * LANES:(t + 1) * LANES]

            if l == 0 and r == 0:
                ld[0]['lens'].wait()
            ld[l][f'k{r}'].wait()
            ld[l][f'v{r}'].wait()
            stats = [jnp.zeros((SUB, LANES), F32) for _ in range(2)]
            for bb in range(SUB):
                b = r * SUB + bb
                xq = qs[r, bb * nc:(bb + 1) * nc, :]
                xr = pltpu.roll(xq, dh, 1)
                z = jnp.zeros((SUB, LANES), F32)
                parts = []
                for a, o in ((xq, xr), (xr, xq)):
                    e0 = jnp.where(ma, a[0:SUB], jnp.where(mb, o[0:SUB], 0.0))
                    e1 = jnp.where(ma, a[SUB:], jnp.where(mb, o[SUB:], 0.0))
                    parts.append(jnp.concatenate([e0, z], axis=1))
                    parts.append(jnp.concatenate([z, e1], axis=1))
                qf = jnp.concatenate(parts, axis=0)
                pb = lens_v[b] - 1 - off
                s = _dot(qf.astype(BF16), k_v[l, b]) * dh ** -0.5
                sn = jnp.sum(qf * kn[r, bb:bb + 1, :], axis=1, keepdims=True) * dh ** -0.5
                s = jnp.where(col < pb, s, jnp.where(col == pb, sn, -jnp.inf))
                m = jnp.maximum(jnp.max(s, axis=1, keepdims=True), NEG)
                p = jnp.exp(s - m)
                den = jnp.sum(p, axis=1, keepdims=True)
                inside = jnp.logical_and(pb >= 0, pb < s_dev)
                pn = jnp.where(inside, jnp.exp(sn - m), 0.0)
                pz = jnp.where(col == pb, 0.0, p).astype(BF16)
                o = lax.dot_general(pz, v_v[l, b], (((1,), (1,)), ((), ())), preferred_element_type=F32)
                o = o + pn * vn[r, bb:bb + 1, :]
                for t in range(2):
                    te, to = slice(t * SUB, (t + 1) * SUB), slice(nc + t * SUB, nc + (t + 1) * SUB)
                    ev = o[te, t * LANES:(t + 1) * LANES]
                    od = o[to, t * LANES:(t + 1) * LANES]
                    evr = pltpu.roll(ev, dh, 1)
                    odr = pltpu.roll(od, dh, 1)
                    os[l, r, pl.ds(t * SUB * SUB + bb, SUB, stride=SUB), :] = jnp.where(
                        row < SUB // 2, jnp.where(lo, ev, odr), jnp.where(lo, evr, od))
                    for i, val in enumerate((m[te], den[te], m[to], den[to])):
                        stats[t] = jnp.where(lane == i * STW + bb, val, stats[t])
            for t in range(2):
                ss[l, r, t * SUB:(t + 1) * SUB, :] = stats[t]
            if l == 0 and r == 0:
                pl.semaphore_wait(bar, n - 1)
            to_owners([(lambda c: os.at[l, r, pl.ds(pl.multiple_of(c * SUB, SUB), SUB)], orv.at[l, r, me], sem(l, r, A2A)),
                       (lambda c: ss.at[l, r, pl.ds(c, 1)], sr.at[l, r, pl.ds(me, 1)], sem(l, r, STAT))])

        if l == 0:
            @pl.when(jnp.logical_not(own))
            def _():
                for c in wo_in:
                    c.start()

            @pl.when(own)
            def _():
                for c in wo_my:
                    c.start()
            for ll in range(1, nl):
                for c in ld[ll].values():
                    c.start()
        pad = jnp.zeros((LANES - nb, kvd), F32)
        knt[...] = jnp.concatenate([kn[0], kn[1], pad], axis=0).T
        vnt[...] = jnp.concatenate([vn[0], vn[1], pad], axis=0).T
        put_new(l, knt, k_v)

        @pl.when(own)
        def _():
            for r in range(2):
                orv[l, r, me] = os[l, r, pl.ds(pl.multiple_of(mc * SUB, SUB), SUB), :]
                sr[l, r, pl.ds(me, 1), :] = ss[l, r, pl.ds(mc, 1), :]
                wait(orv.at[l, r], n - 1, rsem.at[sem(l, r, A2A)])
                wait(sr.at[l, r], n - 1, rsem.at[sem(l, r, STAT)])
                sa = sr[l, r]
                w = jnp.exp(sa - jnp.max(sa, axis=0, keepdims=True))
                den = jnp.sum(w * pltpu.roll(sa, LANES - STW, 1), axis=0, keepdims=True)
                cf = jnp.concatenate([w / den, jnp.zeros((LANES - n, LANES), F32)], axis=0).T
                acc = jnp.zeros((SUB, LANES), F32)
                for i in range(n):
                    f = jnp.where(lo, cf[0:SUB, i:i + 1], cf[2 * STW:2 * STW + SUB, i:i + 1])
                    acc = acc + f * orv[l, r, i]
                if r == 0:
                    wo_in[l].wait_recv()
                    wo_my[l].wait()
                part = _dot(acc.astype(BF16), wo_v[l])
                for c in range(nc):
                    s1[l, r, c] = part[:, c * LANES:(c + 1) * LANES]

                def body(k, carry):
                    c = lax.rem(mc + k, nc)
                    rcopy(s1.at[l, r, c], r1.at[l, r, mc], sem(l, r, RS1), 2 * c + OWN).start()
                    return carry
                lax.fori_loop(1, nc, body, 0)
                r1[l, r, mc] = s1[l, r, mc]

        put_new(l, vnt, v_v)

        @pl.when(own)
        def _():
            for r in range(2):
                wait(r1.at[l, r], nc - 1, rsem.at[sem(l, r, RS1)])
                tot = r1[l, r, 0]
                for c in range(1, nc):
                    tot = tot + r1[l, r, c]
                gather(l, st, r, AG1, (hb[0, r, mc] if st == 0 else hs[st - 1, r]) + tot)

        for r in range(2):
            gathered(l, st, r, AG1)
            if r == 0:
                if l == 0:
                    ld[0]['g2'].wait()
                ld[l]['w1'].wait()
                ld[l]['w2'].wait()
            normed(st + 1, r, g2_v, l)
            u = jax.nn.gelu(_dot(xn[r], w1_v[l]), approximate=True).astype(BF16)
            part = _dot(u, w2_v[l])
            for c in range(nc):
                s2[l, r, c] = part[:, c * LANES:(c + 1) * LANES]
            to_owners([(lambda c: s2.at[l, r, c], r2.at[l, r, me], sem(l, r, RS2))])

        @pl.when(own)
        def _():
            for r in range(2):
                r2[l, r, me] = s2[l, r, mc]
                wait(r2.at[l, r], n - 1, rsem.at[sem(l, r, RS2)])
                tot = r2[l, r, 0]
                for d in range(1, n):
                    tot = tot + r2[l, r, d]
                gather(l, st + 1, r, AG2, hs[st, r] + tot)
        st += 2

    for r in range(2):
        gathered(nl - 1, st - 1, r, AG2)
    for c in range(nc):
        y_ref[:, c * LANES:(c + 1) * LANES] = jnp.concatenate([hb[st, 0, c], hb[st, 1, c]], axis=0).astype(BF16)

    @pl.when(own)
    def _():
        for l in range(nl):
            for r in range(2):
                wait(orv.at[l, r], nc - 1, ssem.at[sem(l, r, A2A)])
                wait(sr.at[l, r], nc - 1, ssem.at[sem(l, r, STAT)])
                wait(r1.at[l, r], nc - 1, ssem.at[sem(l, r, RS1)])
                wait(orv.at[l, r], n - 1, ssem.at[sem(l, r, AG1)])
                wait(r1.at[l, r], nc - 1, ssem.at[sem(l, r, RS2)])
                wait(orv.at[l, r], n - 1, ssem.at[sem(l, r, AG2)])

    @pl.when(jnp.logical_not(own))
    def _():
        for l in range(nl):
            wo_in[l].wait_send()
            for r in range(2):
                wait(orv.at[l, r], nc, ssem.at[sem(l, r, A2A)])
                wait(sr.at[l, r], nc, ssem.at[sem(l, r, STAT)])
                wait(r1.at[l, r], nc, ssem.at[sem(l, r, RS2)])


def _cache_kernel(y_ref, k_ref, v_ref, y_out, k_out, v_out, sem):
    cps = [pltpu.make_async_copy(s, d, sem.at[i])
           for i, (s, d) in enumerate(((y_ref, y_out), (k_ref, k_out), (v_ref, v_out)))]
    for c in cps:
        c.start()
    for c in cps:
        c.wait()


def solution(mesh):
    n = mesh.shape['sp']
    kspec = P(None, 'dp', 'sp', None, None)

    def local(x, lens, wq, wk, wv, wo, w1, w2, g1, g2, kc, vc):
        nl, nb, s_dev, kvh, dh = kc.shape
        D = x.shape[1]
        kvd = kvh * dh
        ff = w1.shape[2]
        nc = n // 2
        kt = jnp.transpose(kc, (0, 1, 3, 4, 2)).reshape(nl, nb, kvd, s_dev)
        vt = jnp.transpose(vc, (0, 1, 3, 4, 2)).reshape(nl, nb, kvd, s_dev)
        vm = pl.BlockSpec(memory_space=pltpu.VMEM)
        anys = pl.BlockSpec(memory_space=pl.ANY)
        tile = (SUB, LANES)
        y, ks, vs = pl.pallas_call(
            functools.partial(_step_kernel, n, (nl, nb, s_dev, kvd, dh)),
            out_shape=(pltpu.VMEM((nb, D), BF16), pltpu.VMEM(kt.shape, BF16), pltpu.VMEM(vt.shape, BF16)),
            in_specs=[anys] * 12,
            out_specs=(vm, vm, vm),
            scratch_shapes=[
                pltpu.VMEM((nl, D, D), BF16),
                pltpu.VMEM((nl, D, kvd), BF16),
                pltpu.VMEM((nl, D, kvd), BF16),
                pltpu.VMEM((nl, 2 * dh, D), BF16),
                pltpu.VMEM((nl, D, ff), BF16),
                pltpu.VMEM((nl, ff, D), BF16),
                pltpu.VMEM(x.shape, BF16),
                pltpu.VMEM(g1.shape, BF16),
                pltpu.VMEM(g2.shape, BF16),
                pltpu.SMEM(lens.shape, jnp.int32),
                pltpu.VMEM((2, SUB * nc, LANES), F32),
                pltpu.VMEM((2, SUB, kvd), F32),
                pltpu.VMEM((2, SUB, kvd), F32),
                pltpu.VMEM((kvd, LANES), F32),
                pltpu.VMEM((kvd, LANES), F32),
                pltpu.VMEM((2, SUB, D), BF16),
                pltpu.VMEM((2 * nl + 1, 2, nc) + tile, F32),
                pltpu.VMEM((2 * nl, 2) + tile, F32),
                pltpu.VMEM((nl, 2, nc * SUB, LANES), F32),
                pltpu.VMEM((nl, 2, n) + tile, F32),
                pltpu.VMEM((nl, 2, nc, LANES), F32),
                pltpu.VMEM((nl, 2, n, LANES), F32),
                pltpu.VMEM((nl, 2, nc) + tile, F32),
                pltpu.VMEM((nl, 2, nc) + tile, F32),
                pltpu.VMEM((nl, 2, nc) + tile, F32),
                pltpu.VMEM((nl, 2, n) + tile, F32),
                pltpu.SemaphoreType.DMA((nl, QCH + 13)),
                pltpu.SemaphoreType.DMA((14 * nl,)),
                pltpu.SemaphoreType.DMA((14 * nl,)),
            ],
            compiler_params=pltpu.CompilerParams(
                collective_id=0, has_side_effects=True, vmem_limit_bytes=40 * 1024 * 1024),
        )(lens, x, g1, g2, wq, wk, wv, wo, w1, w2, kt, vt)

        y, k2, v2 = pl.pallas_call(
            _cache_kernel,
            out_shape=(jax.ShapeDtypeStruct((nb, D), BF16), jax.ShapeDtypeStruct(kt.shape, BF16),
                       jax.ShapeDtypeStruct(vt.shape, BF16)),
            in_specs=[vm, vm, vm],
            out_specs=(anys, anys, anys),
            scratch_shapes=[pltpu.SemaphoreType.DMA((3,))],
            compiler_params=pltpu.CompilerParams(vmem_limit_bytes=1024 * 1024),
        )(y, ks, vs)

        def back(a):
            return jnp.transpose(a.reshape(nl, nb, kvh, dh, s_dev), (0, 1, 4, 2, 3))
        return y, back(k2), back(v2)

    return jax.shard_map(
        local, mesh=mesh,
        in_specs=(P('dp', None), P('dp'), P(), P(), P(), P(None, 'sp', None), P(None, None, 'sp'),
                  P(None, 'sp', None), P(), P(), kspec, kspec),
        out_specs=(P('dp', None), kspec, kspec), check_vma=False)
```

```python
import functools

import jax
import jax.numpy as jnp
from jax import lax
from jax.experimental import pallas as pl
from jax.experimental.pallas import tpu as pltpu
from jax.sharding import PartitionSpec as P

EPS = 1e-6
LANES = 128
SUB = 8
NEG = float(jnp.finfo(jnp.float32).min)
F32 = jnp.float32
BF16 = jnp.bfloat16
MESH = pl.DeviceIdType.MESH
QCH = 4
OWN = 1
PIECES = 4
STW = 32


def _dot(a, w):
    return jnp.dot(a, w, preferred_element_type=F32)


def _step_kernel(n, dims, lens, x, g1, g2, wq, wk, wv, wo, w1, w2, kc, vc,
                 y_ref, k_v, v_v,
                 wq_v, wk_v, wv_v, wo_v, w1_v, w2_v, x_v, g1_v, g2_v, lens_v, sc, sns, pc, qs, kv, knt, vnt, xn, hb, hs,
                 ys, yb, os, orv, ss, sr, s1, r1, s2, r2, lsem, ssem, rsem):
    nl, nb, s_dev, kvd, dh = dims
    D = x_v.shape[1]
    nc = n // 2
    me = lax.axis_index('sp')
    par = lax.rem(me, 2)
    mc = lax.div(me, 2)
    own = par == OWN
    other = me + 1 - 2 * par

    cw = D // QCH
    hw = D // 2

    def local_copy(src, dst, l, i):
        return pltpu.make_async_copy(src, dst, lsem.at[l, i])

    hq = hw // QCH
    l_x = [local_copy(s, d, 0, i) for i, (s, d) in enumerate(((x, x_v), (g1, g1_v), (lens, lens_v), (g2, g2_v)))]
    l_k0 = local_copy(wk.at[0], wk_v.at[0], 0, 4)
    l_v0 = local_copy(wv.at[0], wk_v.at[0], 0, 4)
    l_q0 = []
    for j in range(QCH):
        sl = pl.ds(pl.multiple_of(par * hw + j * hq, LANES), hq)
        l_q0.append(local_copy(wq.at[0, :, sl], wq_v.at[0, :, pl.ds(j * hq, hq)], 0, 5 + j))
    l_q1 = [local_copy(wq.at[l, :, pl.ds(j * cw, cw)], wq_v.at[l, :, pl.ds(j * cw, cw)], l, 5 + j)
            for l in range(1, nl) for j in range(QCH)]
    l_q1 += [local_copy(wk.at[l], wk_v.at[l], l, 3) for l in range(1, nl)]
    l_q1 += [local_copy(wv.at[l], wv_v.at[l], l, 4) for l in range(1, nl)]
    o = 5 + QCH
    l_kv = [[[local_copy(a.at[l, pl.ds(r * SUB, SUB)], b.at[l, pl.ds(r * SUB, SUB)], l, o + 2 * r + i)
              for i, (a, b) in enumerate(((kc, k_v), (vc, v_v)))] for r in range(2)] for l in range(nl)]
    l_w = [[local_copy(w1.at[l], w1_v.at[l], l, o + 4), local_copy(w2.at[l], w2_v.at[l], l, o + 5)] for l in range(nl)]

    def start(cs):
        for c in cs:
            c.start()

    def done(cs):
        for c in cs:
            c.wait()

    start(l_x[:3])

    @pl.when(par == 0)
    def _():
        l_k0.start()

    @pl.when(par == 1)
    def _():
        l_v0.start()
    start(l_q0)

    bar = pltpu.get_barrier_semaphore()

    def sig(k, carry):
        pl.semaphore_signal(bar, 1, device_id={'sp': lax.rem(me + k, n)}, device_id_type=MESH)
        return carry
    lax.fori_loop(1, n, sig, 0)

    A2A, STAT, RS1, AG1, RS2, AG2, WO, XQ, XKV = range(9)

    def sem(l, r, kind):
        return (l * 2 + r) * 9 + kind

    def rcopy(src, dst, i, d):
        return pltpu.make_async_remote_copy(src, dst, ssem.at[i], rsem.at[i], device_id={'sp': d}, device_id_type=MESH)

    def to_owners(pairs):
        def body(k, carry):
            c = lax.rem(mc + k, nc)
            for src, dst, i in pairs:
                rcopy(src(c), dst, i, 2 * c + OWN).start()
            return carry
        lax.fori_loop(1, nc, body, 0)

        @pl.when(jnp.logical_not(own))
        def _():
            body(0, 0)

    def wait(ref, count, s):
        r = ref.at[pl.ds(0, count)]
        pltpu.make_async_copy(r, r, s).wait()

    lane = lax.broadcasted_iota(jnp.int32, (SUB, LANES), 1)
    row = lax.broadcasted_iota(jnp.int32, (SUB, LANES), 0)
    lo = lane < dh
    ma = (row < SUB // 2) & lo
    mb = (row >= SUB // 2) & (~lo)
    col = lax.broadcasted_iota(jnp.int32, (2 * nc, s_dev), 1)
    col1 = lax.broadcasted_iota(jnp.int32, (1, s_dev), 1)
    off = me * s_dev

    def normed(st, r, g_v, l):
        ss_ = None
        for c in range(nc):
            t = hb[st, r, c]
            ss_ = t * t if ss_ is None else ss_ + t * t
        rr = lax.rsqrt(jnp.sum(ss_, axis=1, keepdims=True) / D + EPS)
        for c in range(nc):
            g = g_v[l:l + 1, c * LANES:(c + 1) * LANES].astype(F32)
            xn[r * SUB:(r + 1) * SUB, c * LANES:(c + 1) * LANES] = (hb[st, r, c] * rr * g).astype(BF16)

    def gather(l, st, r, kind, h):
        if st == 2 * nl - 1:
            ys[r] = h.astype(BF16)
            src, dst = ys.at[r], yb
        else:
            hs[st, r] = h
            src, dst = hs.at[st, r], hb.at[st + 1]

        def body(k, carry):
            rcopy(src, dst.at[r, mc], sem(l, r, kind), lax.rem(me + k, n)).start()
            return carry
        lax.fori_loop(1, n, body, 0)
        dst[r, mc] = src[...]

    def gathered(l, st, r, kind):
        dst = yb if st == 2 * nl - 1 else hb.at[st + 1]

        @pl.when(own)
        def _():
            wait(dst.at[r], nc - 1, rsem.at[sem(l, r, kind)])

        @pl.when(jnp.logical_not(own))
        def _():
            wait(dst.at[r], nc, rsem.at[sem(l, r, kind)])

    def put_new(l, new_t, ref):
        for b in range(nb):
            pb = lens_v[b] - 1 - off
            hit = jnp.where(col1 == pb, 1.0, 0.0).astype(BF16)
            c = jnp.broadcast_to(new_t[:, b:b + 1], (kvd, LANES)).astype(BF16)
            for t in range(s_dev // LANES):
                sl = slice(t * LANES, (t + 1) * LANES)
                hm = jnp.broadcast_to(hit[:, sl], (kvd, LANES)) > 0.5
                ref[l, b, :, sl] = jnp.where(hm, c, ref[l, b, :, sl])

    def store_q(half, rs, c0, q):
        q = q.astype(BF16).astype(F32)
        for t in range(q.shape[1] // LANES):
            for i, r in enumerate(rs):
                qs[half, r, pl.ds(c0 + t, SUB, stride=SUB), :] = q[i * SUB:(i + 1) * SUB, t * LANES:(t + 1) * LANES]

    def store_kv(i, rs, a):
        kv[i, rs] = a.astype(BF16).astype(F32).reshape(-1, SUB, kvd)

    def qkv(l, r):
        a = xn[r * SUB:(r + 1) * SUB, :]
        store_kv(0, slice(r, r + 1), _dot(a, wk_v[l]))
        store_kv(1, slice(r, r + 1), _dot(a, wv_v[l]))
        for j in range(QCH):
            q = _dot(a, wq_v[l, :, j * cw:(j + 1) * cw])
            store_q(j * cw // hw, (r,), j * (cw // LANES) % SUB, q)

    def scores(l, r):
        z = jnp.zeros((SUB, LANES), F32)
        for bb in range(SUB):
            xq = jnp.concatenate([qs[i, r, bb * SUB:(bb + 1) * SUB, :] for i in range(2)], axis=0)
            xr = pltpu.roll(xq, dh, 1)
            parts = []
            for a, o in ((xq, xr), (xr, xq)):
                e0 = jnp.where(ma, a[0:SUB], jnp.where(mb, o[0:SUB], 0.0))
                e1 = jnp.where(ma, a[SUB:], jnp.where(mb, o[SUB:], 0.0))
                parts.append(jnp.concatenate([e0, z], axis=1))
                parts.append(jnp.concatenate([z, e1], axis=1))
            qf = jnp.concatenate(parts, axis=0)
            sc[r, bb] = _dot(qf.astype(BF16), k_v[l, r * SUB + bb])
            sn = jnp.sum(qf * kv[0, r, bb:bb + 1, :], axis=1, keepdims=True) * dh ** -0.5
            sns[r, bb] = jnp.broadcast_to(sn, (2 * nc, LANES))

    def probs(l, r):
        stats = [jnp.zeros((SUB, LANES), F32) for _ in range(2)]
        for bb in range(SUB):
            pb = lens_v[r * SUB + bb] - 1 - off
            sn = sns[r, bb]
            sn4 = jnp.concatenate([sn] * (s_dev // LANES), axis=1)
            s = sc[r, bb] * dh ** -0.5
            s = jnp.where(col < pb, s, jnp.where(col == pb, sn4, -jnp.inf))
            m = jnp.maximum(jnp.max(s, axis=1, keepdims=True), NEG)
            p = jnp.exp(s - m)
            den = jnp.sum(p, axis=1, keepdims=True)
            inside = jnp.logical_and(pb >= 0, pb < s_dev)
            sns[r, bb] = jnp.where(inside, jnp.exp(sn - m), 0.0)
            pc[r, bb] = jnp.where(col == pb, 0.0, p).astype(BF16)
            for t in range(2):
                te, to = slice(t * SUB, (t + 1) * SUB), slice(nc + t * SUB, nc + (t + 1) * SUB)
                for i, val in enumerate((m[te], den[te], m[to], den[to])):
                    stats[t] = jnp.where(lane == i * STW + bb, val, stats[t])
        for t in range(2):
            ss[l, r, t * SUB:(t + 1) * SUB, :] = stats[t]

    def values(l, r):
        for bb in range(SUB):
            o = lax.dot_general(pc[r, bb], v_v[l, r * SUB + bb], (((1,), (1,)), ((), ())), preferred_element_type=F32)
            pn = sns[r, bb]
            o = o + jnp.concatenate([pn] * (kvd // LANES), axis=1) * kv[1, r, bb:bb + 1, :]
            for t in range(2):
                ev = o[t * SUB:(t + 1) * SUB, t * LANES:(t + 1) * LANES]
                od = o[nc + t * SUB:nc + (t + 1) * SUB, t * LANES:(t + 1) * LANES]
                evr = pltpu.roll(ev, dh, 1)
                odr = pltpu.roll(od, dh, 1)
                os[l, r, pl.ds(t * SUB * SUB + bb, SUB, stride=SUB), :] = jnp.where(
                    row < SUB // 2, jnp.where(lo, ev, odr), jnp.where(lo, evr, od))

    def send_partials(l, r):
        to_owners([(lambda c: os.at[l, r, pl.ds(pl.multiple_of(c * SUB, SUB), SUB)], orv.at[l, r, me], sem(l, r, A2A)),
                   (lambda c: ss.at[l, r, pl.ds(c, 1)], sr.at[l, r, pl.ds(me, 1)], sem(l, r, STAT))])

    done(l_x[:2])
    for c in range(nc):
        for r in range(2):
            hb[0, r, c] = x_v[r * SUB:(r + 1) * SUB, c * LANES:(c + 1) * LANES].astype(F32)

    wo_in = [rcopy(wo.at[ll], wo_v.at[ll, pl.ds((1 - OWN) * dh, dh)], sem(ll, 0, WO), other) for ll in range(nl)]
    wo_my = [pltpu.make_async_copy(wo.at[ll], wo_v.at[ll, pl.ds(OWN * dh, dh)], lsem.at[ll, QCH + 11])
             for ll in range(nl)]
    st = 0
    for l in range(nl):
        if l == 0:
            for r in range(2):
                normed(st, r, g1_v, l)
            l_k0.wait()
            store_kv(par, slice(None), _dot(xn[...], wk_v[0]))
            for j in range(QCH):
                l_q0[j].wait()
                if j == 1:
                    start(l_kv[0][0])
                q = _dot(xn[...], wq_v[0, :, j * hq:(j + 1) * hq])
                store_q(par, (0, 1), j * (hq // LANES), q)
            start(l_kv[0][1])
            pl.semaphore_wait(bar, n - 1)
            swap = [rcopy(b.at[par], b.at[par], sem(0, 0, i), other) for b, i in ((qs, XQ), (kv, XKV))]
            start(swap)
            l_x[2].wait()
            for c in swap:
                c.wait_recv()
            done(l_kv[0][0])
            scores(l, 0)
            done(l_kv[0][1])
            start(l_x[3:])
            start(l_w[0])
            probs(l, 0)
            scores(l, 1)
        else:
            gathered(l - 1, st - 1, 0, AG2)
            normed(st, 0, g1_v, l)
            done(l_q1)
            qkv(l, 0)
            done(l_kv[l][0])
            scores(l, 0)
            gathered(l - 1, st - 1, 1, AG2)
            normed(st, 1, g1_v, l)
            probs(l, 0)
            qkv(l, 1)
        values(l, 0)
        send_partials(l, 0)
        if l > 0:
            done(l_kv[l][1])
            scores(l, 1)
        probs(l, 1)
        values(l, 1)
        send_partials(l, 1)
        if l == 0:
            for c in swap:
                c.wait_send()

        if l == 0:
            @pl.when(jnp.logical_not(own))
            def _():
                for c in wo_in:
                    c.start()

            @pl.when(own)
            def _():
                for c in wo_my:
                    c.start()
            start(l_q1)
            for ll in range(1, nl):
                start(l_kv[ll][0] + l_kv[ll][1] + l_w[ll])
        pad = jnp.zeros((LANES - nb, kvd), F32)
        knt[...] = jnp.concatenate([kv[0, 0], kv[0, 1], pad], axis=0).T
        vnt[...] = jnp.concatenate([kv[1, 0], kv[1, 1], pad], axis=0).T
        put_new(l, knt, k_v)

        @pl.when(own)
        def _():
            for r in range(2):
                orv[l, r, me] = os[l, r, pl.ds(pl.multiple_of(mc * SUB, SUB), SUB), :]
                sr[l, r, pl.ds(me, 1), :] = ss[l, r, pl.ds(mc, 1), :]
                wait(orv.at[l, r], n - 1, rsem.at[sem(l, r, A2A)])
                wait(sr.at[l, r], n - 1, rsem.at[sem(l, r, STAT)])
                sa = sr[l, r]
                w = jnp.exp(sa - jnp.max(sa, axis=0, keepdims=True))
                den = jnp.sum(w * pltpu.roll(sa, LANES - STW, 1), axis=0, keepdims=True)
                cf = jnp.concatenate([w / den, jnp.zeros((LANES - n, LANES), F32)], axis=0).T
                acc = jnp.zeros((SUB, LANES), F32)
                for i in range(n):
                    f = jnp.where(lo, cf[0:SUB, i:i + 1], cf[2 * STW:2 * STW + SUB, i:i + 1])
                    acc = acc + f * orv[l, r, i]
                if r == 0:
                    wo_in[l].wait_recv()
                    wo_my[l].wait()
                part = _dot(acc.astype(BF16), wo_v[l])
                for c in range(nc):
                    s1[l, r, c] = part[:, c * LANES:(c + 1) * LANES]

                def body(k, carry):
                    c = lax.rem(mc + k, nc)
                    rcopy(s1.at[l, r, c], r1.at[l, r, mc], sem(l, r, RS1), 2 * c + OWN).start()
                    return carry
                lax.fori_loop(1, nc, body, 0)
                r1[l, r, mc] = s1[l, r, mc]

        put_new(l, vnt, v_v)

        @pl.when(own)
        def _():
            for r in range(2):
                wait(r1.at[l, r], nc - 1, rsem.at[sem(l, r, RS1)])
                tot = r1[l, r, 0]
                for c in range(1, nc):
                    tot = tot + r1[l, r, c]
                gather(l, st, r, AG1, (hb[0, r, mc] if st == 0 else hs[st - 1, r]) + tot)

        for r in range(2):
            gathered(l, st, r, AG1)
            if r == 0:
                if l == 0:
                    done(l_x[3:])
                done(l_w[l])
            normed(st + 1, r, g2_v, l)
            u = jax.nn.gelu(_dot(xn[r * SUB:(r + 1) * SUB, :], w1_v[l]), approximate=True).astype(BF16)
            part = _dot(u, w2_v[l])
            for c in range(nc):
                s2[l, r, c] = part[:, c * LANES:(c + 1) * LANES]
            to_owners([(lambda c: s2.at[l, r, c], r2.at[l, r, me], sem(l, r, RS2))])

        @pl.when(own)
        def _():
            for r in range(2):
                r2[l, r, me] = s2[l, r, mc]
                wait(r2.at[l, r], n - 1, rsem.at[sem(l, r, RS2)])
                tot = r2[l, r, 0]
                for d in range(1, n):
                    tot = tot + r2[l, r, d]
                gather(l, st + 1, r, AG2, hs[st, r] + tot)
        st += 2

    for r in range(2):
        gathered(nl - 1, st - 1, r, AG2)
    for c in range(nc):
        y_ref[:, c * LANES:(c + 1) * LANES] = jnp.concatenate([yb[0, c], yb[1, c]], axis=0)

    @pl.when(own)
    def _():
        for l in range(nl):
            for r in range(2):
                wait(orv.at[l, r], nc - 1, ssem.at[sem(l, r, A2A)])
                wait(sr.at[l, r], nc - 1, ssem.at[sem(l, r, STAT)])
                wait(r1.at[l, r], nc - 1, ssem.at[sem(l, r, RS1)])
                wait(orv.at[l, r], n - 1, ssem.at[sem(l, r, AG1)])
                wait(r1.at[l, r], nc - 1, ssem.at[sem(l, r, RS2)])
                wait(yb.at[r] if l == nl - 1 else orv.at[l, r], n - 1, ssem.at[sem(l, r, AG2)])

    @pl.when(jnp.logical_not(own))
    def _():
        for l in range(nl):
            wo_in[l].wait_send()
            for r in range(2):
                wait(orv.at[l, r], nc, ssem.at[sem(l, r, A2A)])
                wait(sr.at[l, r], nc, ssem.at[sem(l, r, STAT)])
                wait(r1.at[l, r], nc, ssem.at[sem(l, r, RS2)])


def _cache_kernel(y_ref, k_ref, v_ref, y_out, k_out, v_out, sem):
    cps = [pltpu.make_async_copy(y_ref, y_out, sem.at[0])]
    for a, b in ((k_ref, k_out), (v_ref, v_out)):
        for l in range(a.shape[0]):
            for i in range(PIECES):
                sl = pl.ds(i * (a.shape[1] // PIECES), a.shape[1] // PIECES)
                cps.append(pltpu.make_async_copy(a.at[l, sl], b.at[l, sl], sem.at[len(cps)]))
    for c in cps:
        c.start()
    for c in cps:
        c.wait()


def solution(mesh):
    n = mesh.shape['sp']
    kspec = P(None, 'dp', 'sp', None, None)

    def local(x, lens, wq, wk, wv, wo, w1, w2, g1, g2, kc, vc):
        nl, nb, s_dev, kvh, dh = kc.shape
        D = x.shape[1]
        kvd = kvh * dh
        ff = w1.shape[2]
        nc = n // 2
        kt = jnp.transpose(kc, (0, 1, 3, 4, 2)).reshape(nl, nb, kvd, s_dev)
        vt = jnp.transpose(vc, (0, 1, 3, 4, 2)).reshape(nl, nb, kvd, s_dev)
        vm = pl.BlockSpec(memory_space=pltpu.VMEM)
        anys = pl.BlockSpec(memory_space=pl.ANY)
        tile = (SUB, LANES)
        y, ks, vs = pl.pallas_call(
            functools.partial(_step_kernel, n, (nl, nb, s_dev, kvd, dh)),
            out_shape=(pltpu.VMEM((nb, D), BF16), pltpu.VMEM(kt.shape, BF16), pltpu.VMEM(vt.shape, BF16)),
            in_specs=[anys] * 12,
            out_specs=(vm, vm, vm),
            scratch_shapes=[
                pltpu.VMEM((nl, D, D), BF16),
                pltpu.VMEM((nl, D, kvd), BF16),
                pltpu.VMEM((nl, D, kvd), BF16),
                pltpu.VMEM((nl, 2 * dh, D), BF16),
                pltpu.VMEM((nl, D, ff), BF16),
                pltpu.VMEM((nl, ff, D), BF16),
                pltpu.VMEM(x.shape, BF16),
                pltpu.VMEM(g1.shape, BF16),
                pltpu.VMEM(g2.shape, BF16),
                pltpu.SMEM(lens.shape, jnp.int32),
                pltpu.VMEM((2, SUB, 2 * nc, s_dev), F32),
                pltpu.VMEM((2, SUB, 2 * nc, LANES), F32),
                pltpu.VMEM((2, SUB, 2 * nc, s_dev), BF16),
                pltpu.VMEM((2, 2, SUB * nc // 2, LANES), F32),
                pltpu.VMEM((2, 2, SUB, kvd), F32),
                pltpu.VMEM((kvd, LANES), F32),
                pltpu.VMEM((kvd, LANES), F32),
                pltpu.VMEM((nb, D), BF16),
                pltpu.VMEM((2 * nl, 2, nc) + tile, F32),
                pltpu.VMEM((2 * nl - 1, 2) + tile, F32),
                pltpu.VMEM((2,) + tile, BF16),
                pltpu.VMEM((2, n) + tile, BF16),
                pltpu.VMEM((nl, 2, nc * SUB, LANES), F32),
                pltpu.VMEM((nl, 2, n) + tile, F32),
                pltpu.VMEM((nl, 2, nc, LANES), F32),
                pltpu.VMEM((nl, 2, n, LANES), F32),
                pltpu.VMEM((nl, 2, nc) + tile, F32),
                pltpu.VMEM((nl, 2, nc) + tile, F32),
                pltpu.VMEM((nl, 2, nc) + tile, F32),
                pltpu.VMEM((nl, 2, n) + tile, F32),
                pltpu.SemaphoreType.DMA((nl, QCH + 12)),
                pltpu.SemaphoreType.DMA((18 * nl,)),
                pltpu.SemaphoreType.DMA((18 * nl,)),
            ],
            compiler_params=pltpu.CompilerParams(
                collective_id=0, has_side_effects=True, vmem_limit_bytes=40 * 1024 * 1024),
        )(lens, x, g1, g2, wq, wk, wv, wo, w1, w2, kt, vt)

        y, k2, v2 = pl.pallas_call(
            _cache_kernel,
            out_shape=(jax.ShapeDtypeStruct((nb, D), BF16), jax.ShapeDtypeStruct(kt.shape, BF16),
                       jax.ShapeDtypeStruct(vt.shape, BF16)),
            in_specs=[vm, vm, vm],
            out_specs=(anys, anys, anys),
            scratch_shapes=[pltpu.SemaphoreType.DMA((1 + 2 * nl * PIECES,))],
            compiler_params=pltpu.CompilerParams(vmem_limit_bytes=1024 * 1024),
        )(y, ks, vs)

        def back(a):
            return jnp.transpose(a.reshape(nl, nb, kvh, dh, s_dev), (0, 1, 4, 2, 3))
        return y, back(k2), back(v2)

    return jax.shard_map(
        local, mesh=mesh,
        in_specs=(P('dp', None), P('dp'), P(), P(), P(), P(None, 'sp', None), P(None, None, 'sp'),
                  P(None, 'sp', None), P(), P(), kspec, kspec),
        out_specs=(P('dp', None), kspec, kspec), check_vma=False)
```

```python
import functools
import math

import jax
import jax.numpy as jnp
from jax import lax
from jax.experimental import pallas as pl
from jax.experimental.pallas import tpu as pltpu
from jax.sharding import PartitionSpec as P

EPS = 1e-6
LANES = 128
SUB = 8
NEG = float(jnp.finfo(jnp.float32).min)
F32 = jnp.float32
BF16 = jnp.bfloat16
MESH = pl.DeviceIdType.MESH
QCH = 4
OWN = 1
PIECES = 2
STW = 32


def far_first(m):
    core = 1 if m % 4 == 0 and math.isqrt(m) ** 2 == m else 2
    side = math.isqrt(m // core)

    def hops(k):
        y, x = divmod(k // core, side)
        return min(y, side - y) + min(x, side - x)
    return sorted(range(1, m), key=lambda k: -hops(k))


def _dot(a, w):
    return jnp.dot(a, w, preferred_element_type=F32)


def _step_kernel(n, dims, lens, x, g1, g2, wq, wk, wv, wo, w1, w2, kc, vc,
                 y_ref, k_v, v_v,
                 wq_v, wk_v, wv_v, wo_v, w1_v, w2_v, x_v, g1_v, g2_v, lens_v, sc, sns, pc, qs, kv, knt, vnt, xn, hb, hs,
                 ys, yb, os, orv, ss, sr, s1, r1, s2, r2, lsem, ssem, rsem):
    nl, nb, s_dev, kvd, dh = dims
    D = x_v.shape[1]
    nc = n // 2
    me = lax.axis_index('sp')
    par = lax.rem(me, 2)
    mc = lax.div(me, 2)
    own = par == OWN
    other = me + 1 - 2 * par

    cw = D // QCH
    hw = D // 2

    def local_copy(src, dst, l, i):
        return pltpu.make_async_copy(src, dst, lsem.at[l, i])

    hq = hw // QCH
    l_x = [local_copy(s, d, 0, i) for i, (s, d) in enumerate(((x, x_v), (g1, g1_v), (lens, lens_v), (g2, g2_v)))]
    l_k0 = local_copy(wk.at[0], wk_v.at[0], 0, 4)
    l_v0 = local_copy(wv.at[0], wk_v.at[0], 0, 4)
    l_q0 = []
    for j in range(QCH):
        sl = pl.ds(pl.multiple_of(par * hw + j * hq, LANES), hq)
        l_q0.append(local_copy(wq.at[0, :, sl], wq_v.at[0, :, pl.ds(j * hq, hq)], 0, 5 + j))
    l_q1 = [local_copy(wq.at[l, :, pl.ds(j * cw, cw)], wq_v.at[l, :, pl.ds(j * cw, cw)], l, 5 + j)
            for l in range(1, nl) for j in range(QCH)]
    l_q1 += [local_copy(wk.at[l], wk_v.at[l], l, 3) for l in range(1, nl)]
    l_q1 += [local_copy(wv.at[l], wv_v.at[l], l, 4) for l in range(1, nl)]
    o = 5 + QCH
    l_kv = [[[local_copy(a.at[l, pl.ds(r * SUB, SUB)], b.at[l, pl.ds(r * SUB, SUB)], l, o + 2 * r + i)
              for i, (a, b) in enumerate(((kc, k_v), (vc, v_v)))] for r in range(2)] for l in range(nl)]
    l_w = [[local_copy(w1.at[l], w1_v.at[l], l, o + 4), local_copy(w2.at[l], w2_v.at[l], l, o + 5)] for l in range(nl)]

    def start(cs):
        for c in cs:
            c.start()

    def done(cs):
        for c in cs:
            c.wait()

    start(l_x[:3])

    @pl.when(par == 0)
    def _():
        l_k0.start()

    @pl.when(par == 1)
    def _():
        l_v0.start()
    start(l_q0)

    bar = pltpu.get_barrier_semaphore()

    def sig(k, carry):
        pl.semaphore_signal(bar, 1, device_id={'sp': lax.rem(me + k, n)}, device_id_type=MESH)
        return carry
    lax.fori_loop(1, n, sig, 0)

    A2A, STAT, RS1, AG1, RS2, AG2, WO, XQ, XKV = range(9)

    def sem(l, r, kind):
        return (l * 2 + r) * 9 + kind

    def rcopy(src, dst, i, d):
        return pltpu.make_async_remote_copy(src, dst, ssem.at[i], rsem.at[i], device_id={'sp': d}, device_id_type=MESH)

    def to_owners(pairs):
        def body(k, carry):
            c = lax.rem(mc + k, nc)
            for src, dst, i in pairs:
                rcopy(src(c), dst, i, 2 * c + OWN).start()
            return carry
        for k in far_first(nc):
            body(k, 0)

        @pl.when(jnp.logical_not(own))
        def _():
            body(0, 0)

    def wait(ref, count, s):
        r = ref.at[pl.ds(0, count)]
        pltpu.make_async_copy(r, r, s).wait()

    lane = lax.broadcasted_iota(jnp.int32, (SUB, LANES), 1)
    row = lax.broadcasted_iota(jnp.int32, (SUB, LANES), 0)
    lo = lane < dh
    ma = (row < SUB // 2) & lo
    mb = (row >= SUB // 2) & (~lo)
    col = lax.broadcasted_iota(jnp.int32, (2 * nc, s_dev), 1)
    col1 = lax.broadcasted_iota(jnp.int32, (1, s_dev), 1)
    off = me * s_dev

    def normed(st, r, g_v, l):
        ss_ = None
        for c in range(nc):
            t = hb[st, r, c]
            ss_ = t * t if ss_ is None else ss_ + t * t
        rr = lax.rsqrt(jnp.sum(ss_, axis=1, keepdims=True) / D + EPS)
        for c in range(nc):
            g = g_v[l:l + 1, c * LANES:(c + 1) * LANES].astype(F32)
            xn[r * SUB:(r + 1) * SUB, c * LANES:(c + 1) * LANES] = (hb[st, r, c] * rr * g).astype(BF16)

    def gather(l, st, r, kind, h):
        if st == 2 * nl - 1:
            ys[r] = h.astype(BF16)
            src, dst = ys.at[r], yb
        else:
            hs[st, r] = h
            src, dst = hs.at[st, r], hb.at[st + 1]

        def body(k, carry):
            rcopy(src, dst.at[r, mc], sem(l, r, kind), lax.rem(me + k, n)).start()
            return carry
        for k in far_first(n):
            body(k, 0)
        dst[r, mc] = src[...]

    def gathered(l, st, r, kind):
        dst = yb if st == 2 * nl - 1 else hb.at[st + 1]

        @pl.when(own)
        def _():
            wait(dst.at[r], nc - 1, rsem.at[sem(l, r, kind)])

        @pl.when(jnp.logical_not(own))
        def _():
            wait(dst.at[r], nc, rsem.at[sem(l, r, kind)])

    def put_new(l, new_t, ref):
        for b in range(nb):
            pb = lens_v[b] - 1 - off
            hit = jnp.where(col1 == pb, 1.0, 0.0).astype(BF16)
            c = jnp.broadcast_to(new_t[:, b:b + 1], (kvd, LANES)).astype(BF16)
            for t in range(s_dev // LANES):
                sl = slice(t * LANES, (t + 1) * LANES)
                hm = jnp.broadcast_to(hit[:, sl], (kvd, LANES)) > 0.5
                ref[l, b, :, sl] = jnp.where(hm, c, ref[l, b, :, sl])

    def store_q(half, rs, c0, q):
        q = q.astype(BF16).astype(F32)
        for t in range(q.shape[1] // LANES):
            for i, r in enumerate(rs):
                qs[half, r, pl.ds(c0 + t, SUB, stride=SUB), :] = q[i * SUB:(i + 1) * SUB, t * LANES:(t + 1) * LANES]

    def store_kv(i, rs, a):
        kv[i, rs] = a.astype(BF16).astype(F32).reshape(-1, SUB, kvd)

    def qkv(l, r):
        a = xn[r * SUB:(r + 1) * SUB, :]
        store_kv(0, slice(r, r + 1), _dot(a, wk_v[l]))
        store_kv(1, slice(r, r + 1), _dot(a, wv_v[l]))
        for j in range(QCH):
            q = _dot(a, wq_v[l, :, j * cw:(j + 1) * cw])
            store_q(j * cw // hw, (r,), j * (cw // LANES) % SUB, q)

    def scores(l, r):
        z = jnp.zeros((SUB, LANES), F32)
        for bb in range(SUB):
            xq = jnp.concatenate([qs[i, r, bb * SUB:(bb + 1) * SUB, :] for i in range(2)], axis=0)
            xr = pltpu.roll(xq, dh, 1)
            parts = []
            for a, o in ((xq, xr), (xr, xq)):
                e0 = jnp.where(ma, a[0:SUB], jnp.where(mb, o[0:SUB], 0.0))
                e1 = jnp.where(ma, a[SUB:], jnp.where(mb, o[SUB:], 0.0))
                parts.append(jnp.concatenate([e0, z], axis=1))
                parts.append(jnp.concatenate([z, e1], axis=1))
            qf = jnp.concatenate(parts, axis=0)
            sc[r, bb] = _dot(qf.astype(BF16), k_v[l, r * SUB + bb])
            sn = jnp.sum(qf * kv[0, r, bb:bb + 1, :], axis=1, keepdims=True) * dh ** -0.5
            sns[r, bb] = jnp.broadcast_to(sn, (2 * nc, LANES))

    def probs(l, r):
        stats = [jnp.zeros((SUB, LANES), F32) for _ in range(2)]
        for bb in range(SUB):
            pb = lens_v[r * SUB + bb] - 1 - off
            sn = sns[r, bb]
            sn4 = jnp.concatenate([sn] * (s_dev // LANES), axis=1)
            s = sc[r, bb] * dh ** -0.5
            s = jnp.where(col < pb, s, jnp.where(col == pb, sn4, -jnp.inf))
            m = jnp.maximum(jnp.max(s, axis=1, keepdims=True), NEG)
            p = jnp.exp(s - m)
            den = jnp.sum(p, axis=1, keepdims=True)
            inside = jnp.logical_and(pb >= 0, pb < s_dev)
            sns[r, bb] = jnp.where(inside, jnp.exp(sn - m), 0.0)
            pc[r, bb] = jnp.where(col == pb, 0.0, p).astype(BF16)
            for t in range(2):
                te, to = slice(t * SUB, (t + 1) * SUB), slice(nc + t * SUB, nc + (t + 1) * SUB)
                for i, val in enumerate((m[te], den[te], m[to], den[to])):
                    stats[t] = jnp.where(lane == i * STW + bb, val, stats[t])
        for t in range(2):
            ss[l, r, t * SUB:(t + 1) * SUB, :] = stats[t]

    def values(l, r):
        for bb in range(SUB):
            o = lax.dot_general(pc[r, bb], v_v[l, r * SUB + bb], (((1,), (1,)), ((), ())), preferred_element_type=F32)
            pn = sns[r, bb]
            o = o + jnp.concatenate([pn] * (kvd // LANES), axis=1) * kv[1, r, bb:bb + 1, :]
            for t in range(2):
                ev = o[t * SUB:(t + 1) * SUB, t * LANES:(t + 1) * LANES]
                od = o[nc + t * SUB:nc + (t + 1) * SUB, t * LANES:(t + 1) * LANES]
                evr = pltpu.roll(ev, dh, 1)
                odr = pltpu.roll(od, dh, 1)
                os[l, r, pl.ds(t * SUB * SUB + bb, SUB, stride=SUB), :] = jnp.where(
                    row < SUB // 2, jnp.where(lo, ev, odr), jnp.where(lo, evr, od))

    def send_partials(l, r):
        to_owners([(lambda c: os.at[l, r, pl.ds(pl.multiple_of(c * SUB, SUB), SUB)], orv.at[l, r, me], sem(l, r, A2A)),
                   (lambda c: ss.at[l, r, pl.ds(c, 1)], sr.at[l, r, pl.ds(me, 1)], sem(l, r, STAT))])

    done(l_x[:2])
    for c in range(nc):
        for r in range(2):
            hb[0, r, c] = x_v[r * SUB:(r + 1) * SUB, c * LANES:(c + 1) * LANES].astype(F32)

    wo_in = [rcopy(wo.at[ll], wo_v.at[ll, pl.ds((1 - OWN) * dh, dh)], sem(ll, 0, WO), other) for ll in range(nl)]
    wo_my = [pltpu.make_async_copy(wo.at[ll], wo_v.at[ll, pl.ds(OWN * dh, dh)], lsem.at[ll, QCH + 11])
             for ll in range(nl)]
    st = 0
    for l in range(nl):
        if l == 0:
            for r in range(2):
                normed(st, r, g1_v, l)
            l_k0.wait()
            store_kv(par, slice(None), _dot(xn[...], wk_v[0]))
            for j in range(QCH):
                l_q0[j].wait()
                if j == 1:
                    start(l_kv[0][0])
                q = _dot(xn[...], wq_v[0, :, j * hq:(j + 1) * hq])
                store_q(par, (0, 1), j * (hq // LANES), q)
            start(l_kv[0][1])
            pl.semaphore_wait(bar, n - 1)
            swap = [rcopy(b.at[par], b.at[par], sem(0, 0, i), other) for b, i in ((qs, XQ), (kv, XKV))]
            start(swap)
            l_x[2].wait()
            for c in swap:
                c.wait_recv()
            done(l_kv[0][0])
            scores(l, 0)
            done(l_kv[0][1])
            start(l_x[3:])
            start(l_w[0])
            probs(l, 0)
            scores(l, 1)
        else:
            gathered(l - 1, st - 1, 0, AG2)
            normed(st, 0, g1_v, l)
            done(l_q1)
            qkv(l, 0)
            done(l_kv[l][0])
            scores(l, 0)
            gathered(l - 1, st - 1, 1, AG2)
            normed(st, 1, g1_v, l)
            probs(l, 0)
            qkv(l, 1)
        values(l, 0)
        send_partials(l, 0)
        if l > 0:
            done(l_kv[l][1])
            scores(l, 1)
        probs(l, 1)
        values(l, 1)
        send_partials(l, 1)
        if l == 0:
            for c in swap:
                c.wait_send()

        if l == 0:
            @pl.when(jnp.logical_not(own))
            def _():
                for c in wo_in:
                    c.start()

            @pl.when(own)
            def _():
                for c in wo_my:
                    c.start()
            start(l_q1)
            for ll in range(1, nl):
                start(l_kv[ll][0] + l_kv[ll][1] + l_w[ll])
        pad = jnp.zeros((LANES - nb, kvd), F32)
        knt[...] = jnp.concatenate([kv[0, 0], kv[0, 1], pad], axis=0).T
        vnt[...] = jnp.concatenate([kv[1, 0], kv[1, 1], pad], axis=0).T
        put_new(l, knt, k_v)

        @pl.when(own)
        def _():
            for r in range(2):
                orv[l, r, me] = os[l, r, pl.ds(pl.multiple_of(mc * SUB, SUB), SUB), :]
                sr[l, r, pl.ds(me, 1), :] = ss[l, r, pl.ds(mc, 1), :]
                wait(orv.at[l, r], n - 1, rsem.at[sem(l, r, A2A)])
                wait(sr.at[l, r], n - 1, rsem.at[sem(l, r, STAT)])
                sa = sr[l, r]
                w = jnp.exp(sa - jnp.max(sa, axis=0, keepdims=True))
                den = jnp.sum(w * pltpu.roll(sa, LANES - STW, 1), axis=0, keepdims=True)
                cf = jnp.concatenate([w / den, jnp.zeros((LANES - n, LANES), F32)], axis=0).T
                acc = jnp.zeros((SUB, LANES), F32)
                for i in range(n):
                    f = jnp.where(lo, cf[0:SUB, i:i + 1], cf[2 * STW:2 * STW + SUB, i:i + 1])
                    acc = acc + f * orv[l, r, i]
                if r == 0:
                    wo_in[l].wait_recv()
                    wo_my[l].wait()
                part = _dot(acc.astype(BF16), wo_v[l])
                for c in range(nc):
                    s1[l, r, c] = part[:, c * LANES:(c + 1) * LANES]

                def body(k, carry):
                    c = lax.rem(mc + k, nc)
                    rcopy(s1.at[l, r, c], r1.at[l, r, mc], sem(l, r, RS1), 2 * c + OWN).start()
                    return carry
                for k in far_first(nc):
                    body(k, 0)
                r1[l, r, mc] = s1[l, r, mc]

        put_new(l, vnt, v_v)

        @pl.when(own)
        def _():
            for r in range(2):
                wait(r1.at[l, r], nc - 1, rsem.at[sem(l, r, RS1)])
                tot = r1[l, r, 0]
                for c in range(1, nc):
                    tot = tot + r1[l, r, c]
                gather(l, st, r, AG1, (hb[0, r, mc] if st == 0 else hs[st - 1, r]) + tot)

        for r in range(2):
            gathered(l, st, r, AG1)
            if r == 0:
                if l == 0:
                    done(l_x[3:])
                done(l_w[l])
            normed(st + 1, r, g2_v, l)
            u = jax.nn.gelu(_dot(xn[r * SUB:(r + 1) * SUB, :], w1_v[l]), approximate=True).astype(BF16)
            part = _dot(u, w2_v[l])
            for c in range(nc):
                s2[l, r, c] = part[:, c * LANES:(c + 1) * LANES]
            to_owners([(lambda c: s2.at[l, r, c], r2.at[l, r, me], sem(l, r, RS2))])

        @pl.when(own)
        def _():
            for r in range(2):
                r2[l, r, me] = s2[l, r, mc]
                wait(r2.at[l, r], n - 1, rsem.at[sem(l, r, RS2)])
                tot = r2[l, r, 0]
                for d in range(1, n):
                    tot = tot + r2[l, r, d]
                gather(l, st + 1, r, AG2, hs[st, r] + tot)
        st += 2

    for r in range(2):
        gathered(nl - 1, st - 1, r, AG2)
    for c in range(nc):
        y_ref[:, c * LANES:(c + 1) * LANES] = jnp.concatenate([yb[0, c], yb[1, c]], axis=0)

    @pl.when(own)
    def _():
        for l in range(nl):
            for r in range(2):
                wait(orv.at[l, r], nc - 1, ssem.at[sem(l, r, A2A)])
                wait(sr.at[l, r], nc - 1, ssem.at[sem(l, r, STAT)])
                wait(r1.at[l, r], nc - 1, ssem.at[sem(l, r, RS1)])
                wait(orv.at[l, r], n - 1, ssem.at[sem(l, r, AG1)])
                wait(r1.at[l, r], nc - 1, ssem.at[sem(l, r, RS2)])
                wait(yb.at[r] if l == nl - 1 else orv.at[l, r], n - 1, ssem.at[sem(l, r, AG2)])

    @pl.when(jnp.logical_not(own))
    def _():
        for l in range(nl):
            wo_in[l].wait_send()
            for r in range(2):
                wait(orv.at[l, r], nc, ssem.at[sem(l, r, A2A)])
                wait(sr.at[l, r], nc, ssem.at[sem(l, r, STAT)])
                wait(r1.at[l, r], nc, ssem.at[sem(l, r, RS2)])


def _cache_kernel(y_ref, k_ref, v_ref, y_out, k_out, v_out, sem):
    cps = [pltpu.make_async_copy(y_ref, y_out, sem.at[0])]
    for a, b in ((k_ref, k_out), (v_ref, v_out)):
        for l in range(a.shape[0]):
            for i in range(PIECES):
                sl = pl.ds(i * (a.shape[1] // PIECES), a.shape[1] // PIECES)
                cps.append(pltpu.make_async_copy(a.at[l, sl], b.at[l, sl], sem.at[len(cps)]))
    for c in cps:
        c.start()
    for c in cps:
        c.wait()


def solution(mesh):
    n = mesh.shape['sp']
    kspec = P(None, 'dp', 'sp', None, None)

    def local(x, lens, wq, wk, wv, wo, w1, w2, g1, g2, kc, vc):
        nl, nb, s_dev, kvh, dh = kc.shape
        D = x.shape[1]
        kvd = kvh * dh
        ff = w1.shape[2]
        nc = n // 2
        kt = jnp.transpose(kc, (0, 1, 3, 4, 2)).reshape(nl, nb, kvd, s_dev)
        vt = jnp.transpose(vc, (0, 1, 3, 4, 2)).reshape(nl, nb, kvd, s_dev)
        vm = pl.BlockSpec(memory_space=pltpu.VMEM)
        anys = pl.BlockSpec(memory_space=pl.ANY)
        tile = (SUB, LANES)
        y, ks, vs = pl.pallas_call(
            functools.partial(_step_kernel, n, (nl, nb, s_dev, kvd, dh)),
            out_shape=(pltpu.VMEM((nb, D), BF16), pltpu.VMEM(kt.shape, BF16), pltpu.VMEM(vt.shape, BF16)),
            in_specs=[anys] * 12,
            out_specs=(vm, vm, vm),
            scratch_shapes=[
                pltpu.VMEM((nl, D, D), BF16),
                pltpu.VMEM((nl, D, kvd), BF16),
                pltpu.VMEM((nl, D, kvd), BF16),
                pltpu.VMEM((nl, 2 * dh, D), BF16),
                pltpu.VMEM((nl, D, ff), BF16),
                pltpu.VMEM((nl, ff, D), BF16),
                pltpu.VMEM(x.shape, BF16),
                pltpu.VMEM(g1.shape, BF16),
                pltpu.VMEM(g2.shape, BF16),
                pltpu.SMEM(lens.shape, jnp.int32),
                pltpu.VMEM((2, SUB, 2 * nc, s_dev), F32),
                pltpu.VMEM((2, SUB, 2 * nc, LANES), F32),
                pltpu.VMEM((2, SUB, 2 * nc, s_dev), BF16),
                pltpu.VMEM((2, 2, SUB * nc // 2, LANES), F32),
                pltpu.VMEM((2, 2, SUB, kvd), F32),
                pltpu.VMEM((kvd, LANES), F32),
                pltpu.VMEM((kvd, LANES), F32),
                pltpu.VMEM((nb, D), BF16),
                pltpu.VMEM((2 * nl, 2, nc) + tile, F32),
                pltpu.VMEM((2 * nl - 1, 2) + tile, F32),
                pltpu.VMEM((2,) + tile, BF16),
                pltpu.VMEM((2, n) + tile, BF16),
                pltpu.VMEM((nl, 2, nc * SUB, LANES), F32),
                pltpu.VMEM((nl, 2, n) + tile, F32),
                pltpu.VMEM((nl, 2, nc, LANES), F32),
                pltpu.VMEM((nl, 2, n, LANES), F32),
                pltpu.VMEM((nl, 2, nc) + tile, F32),
                pltpu.VMEM((nl, 2, nc) + tile, F32),
                pltpu.VMEM((nl, 2, nc) + tile, F32),
                pltpu.VMEM((nl, 2, n) + tile, F32),
                pltpu.SemaphoreType.DMA((nl, QCH + 12)),
                pltpu.SemaphoreType.DMA((18 * nl,)),
                pltpu.SemaphoreType.DMA((18 * nl,)),
            ],
            compiler_params=pltpu.CompilerParams(
                collective_id=0, has_side_effects=True, vmem_limit_bytes=40 * 1024 * 1024),
        )(lens, x, g1, g2, wq, wk, wv, wo, w1, w2, kt, vt)

        y, k2, v2 = pl.pallas_call(
            _cache_kernel,
            out_shape=(jax.ShapeDtypeStruct((nb, D), BF16), jax.ShapeDtypeStruct(kt.shape, BF16),
                       jax.ShapeDtypeStruct(vt.shape, BF16)),
            in_specs=[vm, vm, vm],
            out_specs=(anys, anys, anys),
            scratch_shapes=[pltpu.SemaphoreType.DMA((1 + 2 * nl * PIECES,))],
            compiler_params=pltpu.CompilerParams(vmem_limit_bytes=1024 * 1024),
        )(y, ks, vs)

        def back(a):
            return jnp.transpose(a.reshape(nl, nb, kvh, dh, s_dev), (0, 1, 4, 2, 3))
        return y, back(k2), back(v2)

    return jax.shard_map(
        local, mesh=mesh,
        in_specs=(P('dp', None), P('dp'), P(), P(), P(), P(None, 'sp', None), P(None, None, 'sp'),
                  P(None, 'sp', None), P(), P(), kspec, kspec),
        out_specs=(P('dp', None), kspec, kspec), check_vma=False)
```

```python
import functools
import math

import jax
import jax.numpy as jnp
from jax import lax
from jax.experimental import pallas as pl
from jax.experimental.pallas import tpu as pltpu
from jax.sharding import PartitionSpec as P

EPS = 1e-6
LANES = 128
SUB = 8
NEG = float(jnp.finfo(jnp.float32).min)
F32 = jnp.float32
BF16 = jnp.bfloat16
MESH = pl.DeviceIdType.MESH
QCH = 4
OWN = 1
PIECES = 2
MSG = 2 * SUB
STW = 32


def far_first(m):
    core = 1 if m % 4 == 0 and math.isqrt(m) ** 2 == m else 2
    side = math.isqrt(m // core)

    def hops(k):
        y, x = divmod(k // core, side)
        return min(y, side - y) + min(x, side - x)
    return sorted(range(1, m), key=lambda k: -hops(k))


def _dot(a, w):
    return jnp.dot(a, w, preferred_element_type=F32)


def _step_kernel(n, dims, lens, x, g1, g2, wq, wk, wv, wo, w1, w2, kc, vc,
                 y_ref, k_v, v_v,
                 wq_v, wk_v, wv_v, wo_v, w1_v, w2_v, x_v, g1_v, g2_v, lens_v, sc, sns, pc, qs, kv, knt, vnt, xn, hb, hs,
                 ys, yb, os, orv, s1, r1, s2, r2, lsem, ssem, rsem):
    nl, nb, s_dev, kvd, dh = dims
    D = x_v.shape[1]
    nc = n // 2
    me = lax.axis_index('sp')
    par = lax.rem(me, 2)
    mc = lax.div(me, 2)
    own = par == OWN
    other = me + 1 - 2 * par

    cw = D // QCH
    hw = D // 2

    def local_copy(src, dst, l, i):
        return pltpu.make_async_copy(src, dst, lsem.at[l, i])

    hq = hw // QCH
    l_x = [local_copy(s, d, 0, i) for i, (s, d) in enumerate(((x, x_v), (g1, g1_v), (lens, lens_v), (g2, g2_v)))]
    l_k0 = local_copy(wk.at[0], wk_v.at[0], 0, 4)
    l_v0 = local_copy(wv.at[0], wk_v.at[0], 0, 4)
    l_q0 = []
    for j in range(QCH):
        sl = pl.ds(pl.multiple_of(par * hw + j * hq, LANES), hq)
        l_q0.append(local_copy(wq.at[0, :, sl], wq_v.at[0, :, pl.ds(j * hq, hq)], 0, 5 + j))
    l_q1 = [local_copy(wq.at[l, :, pl.ds(j * cw, cw)], wq_v.at[l, :, pl.ds(j * cw, cw)], l, 5 + j)
            for l in range(1, nl) for j in range(QCH)]
    l_q1 += [local_copy(wk.at[l], wk_v.at[l], l, 3) for l in range(1, nl)]
    l_q1 += [local_copy(wv.at[l], wv_v.at[l], l, 4) for l in range(1, nl)]
    o = 5 + QCH
    l_kv = [[[local_copy(a.at[l, pl.ds(r * SUB, SUB)], b.at[l, pl.ds(r * SUB, SUB)], l, o + 2 * r + i)
              for i, (a, b) in enumerate(((kc, k_v), (vc, v_v)))] for r in range(2)] for l in range(nl)]
    l_w = [[local_copy(w1.at[l], w1_v.at[l], l, o + 4), local_copy(w2.at[l], w2_v.at[l], l, o + 5)] for l in range(nl)]

    def start(cs):
        for c in cs:
            c.start()

    def done(cs):
        for c in cs:
            c.wait()

    start(l_x[:3])

    @pl.when(par == 0)
    def _():
        l_k0.start()

    @pl.when(par == 1)
    def _():
        l_v0.start()
    start(l_q0)

    bar = pltpu.get_barrier_semaphore()

    def sig(k, carry):
        pl.semaphore_signal(bar, 1, device_id={'sp': lax.rem(me + k, n)}, device_id_type=MESH)
        return carry
    lax.fori_loop(1, n, sig, 0)

    A2A, STAT, RS1, AG1, RS2, AG2, WO, XQ, XKV = range(9)

    def sem(l, r, kind):
        return (l * 2 + r) * 9 + kind

    def rcopy(src, dst, i, d):
        return pltpu.make_async_remote_copy(src, dst, ssem.at[i], rsem.at[i], device_id={'sp': d}, device_id_type=MESH)

    def to_owners(pairs):
        def body(k, carry):
            c = lax.rem(mc + k, nc)
            for src, dst, i in pairs:
                rcopy(src(c), dst, i, 2 * c + OWN).start()
            return carry
        for k in far_first(nc):
            body(k, 0)

        @pl.when(jnp.logical_not(own))
        def _():
            body(0, 0)

    def wait(ref, count, s):
        r = ref.at[pl.ds(0, count)]
        pltpu.make_async_copy(r, r, s).wait()

    lane = lax.broadcasted_iota(jnp.int32, (SUB, LANES), 1)
    row = lax.broadcasted_iota(jnp.int32, (SUB, LANES), 0)
    lo = lane < dh
    ma = (row < SUB // 2) & lo
    mb = (row >= SUB // 2) & (~lo)
    col = lax.broadcasted_iota(jnp.int32, (2 * nc, s_dev), 1)
    col1 = lax.broadcasted_iota(jnp.int32, (1, s_dev), 1)
    off = me * s_dev

    def normed(st, r, g_v, l):
        ss_ = None
        for c in range(nc):
            t = hb[st, r, c]
            ss_ = t * t if ss_ is None else ss_ + t * t
        rr = lax.rsqrt(jnp.sum(ss_, axis=1, keepdims=True) / D + EPS)
        for c in range(nc):
            g = g_v[l:l + 1, c * LANES:(c + 1) * LANES].astype(F32)
            xn[r * SUB:(r + 1) * SUB, c * LANES:(c + 1) * LANES] = (hb[st, r, c] * rr * g).astype(BF16)

    def gather(l, st, r, kind, h):
        if st == 2 * nl - 1:
            ys[r] = h.astype(BF16)
            src, dst = ys.at[r], yb
        else:
            hs[st, r] = h
            src, dst = hs.at[st, r], hb.at[st + 1]

        def body(k, carry):
            rcopy(src, dst.at[r, mc], sem(l, r, kind), lax.rem(me + k, n)).start()
            return carry
        for k in far_first(n):
            body(k, 0)
        dst[r, mc] = src[...]

    def gathered(l, st, r, kind):
        dst = yb if st == 2 * nl - 1 else hb.at[st + 1]

        @pl.when(own)
        def _():
            wait(dst.at[r], nc - 1, rsem.at[sem(l, r, kind)])

        @pl.when(jnp.logical_not(own))
        def _():
            wait(dst.at[r], nc, rsem.at[sem(l, r, kind)])

    def put_new(l, new_t, ref):
        for b in range(nb):
            pb = lens_v[b] - 1 - off
            hit = jnp.where(col1 == pb, 1.0, 0.0).astype(BF16)
            c = jnp.broadcast_to(new_t[:, b:b + 1], (kvd, LANES)).astype(BF16)
            for t in range(s_dev // LANES):
                sl = slice(t * LANES, (t + 1) * LANES)
                hm = jnp.broadcast_to(hit[:, sl], (kvd, LANES)) > 0.5
                ref[l, b, :, sl] = jnp.where(hm, c, ref[l, b, :, sl])

    def store_q(half, rs, c0, q):
        q = q.astype(BF16).astype(F32)
        for t in range(q.shape[1] // LANES):
            for i, r in enumerate(rs):
                qs[half, r, pl.ds(c0 + t, SUB, stride=SUB), :] = q[i * SUB:(i + 1) * SUB, t * LANES:(t + 1) * LANES]

    def store_kv(i, rs, a):
        kv[i, rs] = a.astype(BF16).astype(F32).reshape(-1, SUB, kvd)

    def qkv(l, r):
        a = xn[r * SUB:(r + 1) * SUB, :]
        store_kv(0, slice(r, r + 1), _dot(a, wk_v[l]))
        for j in range(QCH):
            q = _dot(a, wq_v[l, :, j * cw:(j + 1) * cw])
            store_q(j * cw // hw, (r,), j * (cw // LANES) % SUB, q)
        store_kv(1, slice(r, r + 1), _dot(a, wv_v[l]))

    def scores(l, r):
        z = jnp.zeros((SUB, LANES), F32)
        for bb in range(SUB):
            xq = jnp.concatenate([qs[i, r, bb * SUB:(bb + 1) * SUB, :] for i in range(2)], axis=0)
            xr = pltpu.roll(xq, dh, 1)
            parts = []
            for a, o in ((xq, xr), (xr, xq)):
                e0 = jnp.where(ma, a[0:SUB], jnp.where(mb, o[0:SUB], 0.0))
                e1 = jnp.where(ma, a[SUB:], jnp.where(mb, o[SUB:], 0.0))
                parts.append(jnp.concatenate([e0, z], axis=1))
                parts.append(jnp.concatenate([z, e1], axis=1))
            qf = jnp.concatenate(parts, axis=0)
            sc[r, bb] = _dot(qf.astype(BF16), k_v[l, r * SUB + bb])
            sn = jnp.sum(qf * kv[0, r, bb:bb + 1, :], axis=1, keepdims=True) * dh ** -0.5
            sns[r, bb] = jnp.broadcast_to(sn, (2 * nc, LANES))

    def probs(l, r):
        stats = [jnp.zeros((SUB, LANES), F32) for _ in range(2)]
        for bb in range(SUB):
            pb = lens_v[r * SUB + bb] - 1 - off
            sn = sns[r, bb]
            sn4 = jnp.concatenate([sn] * (s_dev // LANES), axis=1)
            s = sc[r, bb] * dh ** -0.5
            s = jnp.where(col < pb, s, jnp.where(col == pb, sn4, -jnp.inf))
            m = jnp.maximum(jnp.max(s, axis=1, keepdims=True), NEG)
            p = jnp.exp(s - m)
            den = jnp.sum(p, axis=1, keepdims=True)
            inside = jnp.logical_and(pb >= 0, pb < s_dev)
            sns[r, bb] = jnp.where(inside, jnp.exp(sn - m), 0.0)
            pc[r, bb] = jnp.where(col == pb, 0.0, p).astype(BF16)
            for t in range(2):
                te, to = slice(t * SUB, (t + 1) * SUB), slice(nc + t * SUB, nc + (t + 1) * SUB)
                for i, val in enumerate((m[te], den[te], m[to], den[to])):
                    stats[t] = jnp.where(lane == i * STW + bb, val, stats[t])
        for t in range(2):
            os[l, r, pl.ds(t * SUB * MSG + SUB, SUB, stride=MSG), :] = stats[t]

    def values(l, r):
        for bb in range(SUB):
            o = lax.dot_general(pc[r, bb], v_v[l, r * SUB + bb], (((1,), (1,)), ((), ())), preferred_element_type=F32)
            pn = sns[r, bb]
            o = o + jnp.concatenate([pn] * (kvd // LANES), axis=1) * kv[1, r, bb:bb + 1, :]
            for t in range(2):
                ev = o[t * SUB:(t + 1) * SUB, t * LANES:(t + 1) * LANES]
                od = o[nc + t * SUB:nc + (t + 1) * SUB, t * LANES:(t + 1) * LANES]
                evr = pltpu.roll(ev, dh, 1)
                odr = pltpu.roll(od, dh, 1)
                os[l, r, pl.ds(t * SUB * MSG + bb, SUB, stride=MSG), :] = jnp.where(
                    row < SUB // 2, jnp.where(lo, ev, odr), jnp.where(lo, evr, od))

    def send_partials(l, r):
        to_owners([(lambda c: os.at[l, r, pl.ds(pl.multiple_of(c * MSG, MSG), SUB + 1)],
                    orv.at[l, r, pl.ds(pl.multiple_of(me * MSG, MSG), SUB + 1)], sem(l, r, A2A))])

    done(l_x[:2])
    for c in range(nc):
        for r in range(2):
            hb[0, r, c] = x_v[r * SUB:(r + 1) * SUB, c * LANES:(c + 1) * LANES].astype(F32)

    wo_in = [rcopy(wo.at[ll], wo_v.at[ll, pl.ds((1 - OWN) * dh, dh)], sem(ll, 0, WO), other) for ll in range(nl)]
    wo_my = [pltpu.make_async_copy(wo.at[ll], wo_v.at[ll, pl.ds(OWN * dh, dh)], lsem.at[ll, QCH + 11])
             for ll in range(nl)]
    st = 0
    for l in range(nl):
        if l == 0:
            for r in range(2):
                normed(st, r, g1_v, l)
            l_k0.wait()
            store_kv(par, slice(None), _dot(xn[...], wk_v[0]))
            for j in range(QCH):
                l_q0[j].wait()
                if j == 1:
                    start(l_kv[0][0])
                q = _dot(xn[...], wq_v[0, :, j * hq:(j + 1) * hq])
                store_q(par, (0, 1), j * (hq // LANES), q)
            start(l_kv[0][1])
            pl.semaphore_wait(bar, n - 1)
            swap = [rcopy(b.at[par], b.at[par], sem(0, 0, i), other) for b, i in ((qs, XQ), (kv, XKV))]
            start(swap)
            l_x[2].wait()
            for c in swap:
                c.wait_recv()
            done(l_kv[0][0])
            scores(l, 0)
            done(l_kv[0][1])
            start(l_x[3:])
            start(l_w[0])
            probs(l, 0)
            scores(l, 1)
        else:
            gathered(l - 1, st - 1, 0, AG2)
            normed(st, 0, g1_v, l)
            done(l_q1)
            qkv(l, 0)
            done(l_kv[l][0])
            scores(l, 0)
            gathered(l - 1, st - 1, 1, AG2)
            normed(st, 1, g1_v, l)
            probs(l, 0)
            qkv(l, 1)
        values(l, 0)
        send_partials(l, 0)
        if l > 0:
            done(l_kv[l][1])
            scores(l, 1)
        probs(l, 1)
        values(l, 1)
        send_partials(l, 1)
        if l == 0:
            for c in swap:
                c.wait_send()

        if l == 0:
            @pl.when(jnp.logical_not(own))
            def _():
                for c in wo_in:
                    c.start()

            @pl.when(own)
            def _():
                for c in wo_my:
                    c.start()
            start(l_q1)
            for ll in range(1, nl):
                start(l_kv[ll][0] + l_kv[ll][1] + l_w[ll])
        pad = jnp.zeros((LANES - nb, kvd), F32)
        knt[...] = jnp.concatenate([kv[0, 0], kv[0, 1], pad], axis=0).T
        vnt[...] = jnp.concatenate([kv[1, 0], kv[1, 1], pad], axis=0).T
        put_new(l, knt, k_v)

        @pl.when(own)
        def _():
            for r in range(2):
                for o, k in ((0, SUB), (SUB, 1)):
                    orv[l, r, pl.ds(pl.multiple_of(me * MSG, MSG) + o, k), :] = os[
                        l, r, pl.ds(pl.multiple_of(mc * MSG, MSG) + o, k), :]
                wait(orv.at[l, r], (n - 1) * (SUB + 1), rsem.at[sem(l, r, A2A)])
                sa = orv[l, r, pl.ds(SUB, n, stride=MSG), :]
                w = jnp.exp(sa - jnp.max(sa, axis=0, keepdims=True))
                den = jnp.sum(w * pltpu.roll(sa, LANES - STW, 1), axis=0, keepdims=True)
                cf = jnp.concatenate([w / den, jnp.zeros((LANES - n, LANES), F32)], axis=0).T
                acc = jnp.zeros((SUB, LANES), F32)
                for i in range(n):
                    f = jnp.where(lo, cf[0:SUB, i:i + 1], cf[2 * STW:2 * STW + SUB, i:i + 1])
                    acc = acc + f * orv[l, r, i * MSG:i * MSG + SUB, :]
                if r == 0:
                    wo_in[l].wait_recv()
                    wo_my[l].wait()
                part = _dot(acc.astype(BF16), wo_v[l])
                for c in range(nc):
                    s1[l, r, c] = part[:, c * LANES:(c + 1) * LANES]

                def body(k, carry):
                    c = lax.rem(mc + k, nc)
                    rcopy(s1.at[l, r, c], r1.at[l, r, mc], sem(l, r, RS1), 2 * c + OWN).start()
                    return carry
                for k in far_first(nc):
                    body(k, 0)
                r1[l, r, mc] = s1[l, r, mc]

        put_new(l, vnt, v_v)

        @pl.when(own)
        def _():
            for r in range(2):
                wait(r1.at[l, r], nc - 1, rsem.at[sem(l, r, RS1)])
                tot = r1[l, r, 0]
                for c in range(1, nc):
                    tot = tot + r1[l, r, c]
                gather(l, st, r, AG1, (hb[0, r, mc] if st == 0 else hs[st - 1, r]) + tot)

        for r in range(2):
            gathered(l, st, r, AG1)
            if r == 0:
                if l == 0:
                    done(l_x[3:])
                done(l_w[l])
            normed(st + 1, r, g2_v, l)
            u = jax.nn.gelu(_dot(xn[r * SUB:(r + 1) * SUB, :], w1_v[l]), approximate=True).astype(BF16)
            part = _dot(u, w2_v[l])
            for c in range(nc):
                s2[l, r, c] = part[:, c * LANES:(c + 1) * LANES]
            to_owners([(lambda c: s2.at[l, r, c], r2.at[l, r, me], sem(l, r, RS2))])

        @pl.when(own)
        def _():
            for r in range(2):
                r2[l, r, me] = s2[l, r, mc]
                wait(r2.at[l, r], n - 1, rsem.at[sem(l, r, RS2)])
                tot = r2[l, r, 0]
                for d in range(1, n):
                    tot = tot + r2[l, r, d]
                gather(l, st + 1, r, AG2, hs[st, r] + tot)
        st += 2

    for r in range(2):
        gathered(nl - 1, st - 1, r, AG2)
    for c in range(nc):
        y_ref[:, c * LANES:(c + 1) * LANES] = jnp.concatenate([yb[0, c], yb[1, c]], axis=0)

    @pl.when(own)
    def _():
        for l in range(nl):
            for r in range(2):
                wait(orv.at[l, r], (nc - 1) * (SUB + 1), ssem.at[sem(l, r, A2A)])
                wait(r1.at[l, r], nc - 1, ssem.at[sem(l, r, RS1)])
                wait(r2.at[l, r], n - 1, ssem.at[sem(l, r, AG1)])
                wait(r1.at[l, r], nc - 1, ssem.at[sem(l, r, RS2)])
                wait(yb.at[r] if l == nl - 1 else r2.at[l, r], n - 1, ssem.at[sem(l, r, AG2)])

    @pl.when(jnp.logical_not(own))
    def _():
        for l in range(nl):
            wo_in[l].wait_send()
            for r in range(2):
                wait(orv.at[l, r], nc * (SUB + 1), ssem.at[sem(l, r, A2A)])
                wait(r1.at[l, r], nc, ssem.at[sem(l, r, RS2)])


def _cache_kernel(y_ref, k_ref, v_ref, y_out, k_out, v_out, sem):
    cps = [pltpu.make_async_copy(y_ref, y_out, sem.at[0])]
    for a, b in ((k_ref, k_out), (v_ref, v_out)):
        for l in range(a.shape[0]):
            for i in range(PIECES):
                sl = pl.ds(i * (a.shape[1] // PIECES), a.shape[1] // PIECES)
                cps.append(pltpu.make_async_copy(a.at[l, sl], b.at[l, sl], sem.at[len(cps)]))
    for c in cps:
        c.start()
    for c in cps:
        c.wait()


def solution(mesh):
    n = mesh.shape['sp']
    kspec = P(None, 'dp', 'sp', None, None)

    def local(x, lens, wq, wk, wv, wo, w1, w2, g1, g2, kc, vc):
        nl, nb, s_dev, kvh, dh = kc.shape
        D = x.shape[1]
        kvd = kvh * dh
        ff = w1.shape[2]
        nc = n // 2
        kt = jnp.transpose(kc, (0, 1, 3, 4, 2)).reshape(nl, nb, kvd, s_dev)
        vt = jnp.transpose(vc, (0, 1, 3, 4, 2)).reshape(nl, nb, kvd, s_dev)
        vm = pl.BlockSpec(memory_space=pltpu.VMEM)
        anys = pl.BlockSpec(memory_space=pl.ANY)
        tile = (SUB, LANES)
        y, ks, vs = pl.pallas_call(
            functools.partial(_step_kernel, n, (nl, nb, s_dev, kvd, dh)),
            out_shape=(pltpu.VMEM((nb, D), BF16), pltpu.VMEM(kt.shape, BF16), pltpu.VMEM(vt.shape, BF16)),
            in_specs=[anys] * 12,
            out_specs=(vm, vm, vm),
            scratch_shapes=[
                pltpu.VMEM((nl, D, D), BF16),
                pltpu.VMEM((nl, D, kvd), BF16),
                pltpu.VMEM((nl, D, kvd), BF16),
                pltpu.VMEM((nl, 2 * dh, D), BF16),
                pltpu.VMEM((nl, D, ff), BF16),
                pltpu.VMEM((nl, ff, D), BF16),
                pltpu.VMEM(x.shape, BF16),
                pltpu.VMEM(g1.shape, BF16),
                pltpu.VMEM(g2.shape, BF16),
                pltpu.SMEM(lens.shape, jnp.int32),
                pltpu.VMEM((2, SUB, 2 * nc, s_dev), F32),
                pltpu.VMEM((2, SUB, 2 * nc, LANES), F32),
                pltpu.VMEM((2, SUB, 2 * nc, s_dev), BF16),
                pltpu.VMEM((2, 2, SUB * nc // 2, LANES), F32),
                pltpu.VMEM((2, 2, SUB, kvd), F32),
                pltpu.VMEM((kvd, LANES), F32),
                pltpu.VMEM((kvd, LANES), F32),
                pltpu.VMEM((nb, D), BF16),
                pltpu.VMEM((2 * nl, 2, nc) + tile, F32),
                pltpu.VMEM((2 * nl - 1, 2) + tile, F32),
                pltpu.VMEM((2,) + tile, BF16),
                pltpu.VMEM((2, n) + tile, BF16),
                pltpu.VMEM((nl, 2, nc * MSG, LANES), F32),
                pltpu.VMEM((nl, 2, n * MSG, LANES), F32),
                pltpu.VMEM((nl, 2, nc) + tile, F32),
                pltpu.VMEM((nl, 2, nc) + tile, F32),
                pltpu.VMEM((nl, 2, nc) + tile, F32),
                pltpu.VMEM((nl, 2, n) + tile, F32),
                pltpu.SemaphoreType.DMA((nl, QCH + 12)),
                pltpu.SemaphoreType.DMA((18 * nl,)),
                pltpu.SemaphoreType.DMA((18 * nl,)),
            ],
            compiler_params=pltpu.CompilerParams(
                collective_id=0, has_side_effects=True, vmem_limit_bytes=40 * 1024 * 1024),
        )(lens, x, g1, g2, wq, wk, wv, wo, w1, w2, kt, vt)

        y, k2, v2 = pl.pallas_call(
            _cache_kernel,
            out_shape=(jax.ShapeDtypeStruct((nb, D), BF16), jax.ShapeDtypeStruct(kt.shape, BF16),
                       jax.ShapeDtypeStruct(vt.shape, BF16)),
            in_specs=[vm, vm, vm],
            out_specs=(anys, anys, anys),
            scratch_shapes=[pltpu.SemaphoreType.DMA((1 + 2 * nl * PIECES,))],
            compiler_params=pltpu.CompilerParams(vmem_limit_bytes=1024 * 1024),
        )(y, ks, vs)

        def back(a):
            return jnp.transpose(a.reshape(nl, nb, kvh, dh, s_dev), (0, 1, 4, 2, 3))
        return y, back(k2), back(v2)

    return jax.shard_map(
        local, mesh=mesh,
        in_specs=(P('dp', None), P('dp'), P(), P(), P(), P(None, 'sp', None), P(None, None, 'sp'),
                  P(None, 'sp', None), P(), P(), kspec, kspec),
        out_specs=(P('dp', None), kspec, kspec), check_vma=False)
```
